32 devices in a mesh: freq: 2 (over x), panel: 16 (over z, y, core).
Axes of the slice: x: 2, y: 2, z: 4, core: 2. Of those that a mesh axis runs over, the one named last changes fastest.
Arguments:
- recorded: float32 [2, 2, 2048, 2048], P('freq', None, 'panel'), parts along dimension 0, may hold values from -60 to 60
- receiver_kernel: bfloat16 [2, 2, 4095], P('freq'), parts along dimension 0, may hold values from -1.5 to 1.5
- source_kernel: bfloat16 [2, 2, 4095], P('freq'), parts along dimension 0, may hold values from -1.5 to 1.5
Outputs:
- primaries: float32 [2, 2, 2048, 2048], P('freq', None, 'panel'), parts along dimension 0
- multiples: bfloat16 [2, 2, 2048, 2048], P('freq', None, 'panel'), parts along dimension 0
The draws below stay inside these ranges and needn't reach their ends.
There are 2 independent parts, one for each index of `freq`. The reference program is written for one: setup_inputs(seed, part) draws one part's arguments, and reference() takes and returns one part's arrays. A program takes and returns all parts, laid end to end along the dimension named above; each array names one. Nothing has to cross between parts.
All inputs are finite; a program needn't handle non-finite values.
Results may differ from the reference program's by a relative error of at most 0.0057.
Values may be sent and summed in bfloat16 or wider, within the bound.
No kernel may reach another device: no remote copies, remote signals or barrier semaphores. Data moves between devices by JAX's collectives and lax.ppermute only.
A program may use at most 320 MiB of HBM per device.

```python
import math
import jax
import jax.numpy as jnp

FREQS = 1
NS = 2048
NR = 2048


def focal_kernel(key, width):
    key_taps, key_phase, key_mag = jax.random.split(key, 3)
    count = 2 * width - 1
    taps = jnp.clip(jax.random.normal(key_taps, (FREQS, 2, count), jnp.float32), -6.0, 6.0)
    taps = taps / jnp.sqrt(2.0 * width)
    phase = jax.random.uniform(key_phase, (FREQS, 1), jnp.float32, -math.pi, math.pi)
    magnitude = jax.random.uniform(key_mag, (FREQS, 1), jnp.float32, 0.8, 1.2)
    center = (jnp.arange(count) == width - 1)[None, :]
    real_part = jnp.where(center, magnitude * jnp.cos(phase), taps[:, 0])
    imag_part = jnp.where(center, magnitude * jnp.sin(phase), taps[:, 1])
    return jnp.stack([real_part, imag_part], axis=1).astype(jnp.bfloat16)


def draw_receiver_kernel(key, part):
    return focal_kernel(jax.random.fold_in(key, 11), NR)


def draw_source_kernel(key, part):
    return focal_kernel(jax.random.fold_in(key, 23), NS)


def draw_recorded(key, part):
    key_base, key_rows, key_cols = jax.random.split(jax.random.fold_in(key, 37), 3)
    rising = 3.0 ** (jnp.arange(NS, dtype=jnp.float32) / (NS - 1))
    base = jnp.clip(jax.random.normal(key_base, (FREQS, 2, NS, NR), jnp.float32), -6.0, 6.0)
    row_scale = jnp.exp(jax.random.uniform(key_rows, (NS,), jnp.float32, math.log(0.7), math.log(1.4)))
    col_scale = jnp.exp(jax.random.uniform(key_cols, (NR,), jnp.float32, math.log(0.7), math.log(1.4)))
    return base * (rising * row_scale)[:, None] * col_scale[None, :]


def setup_inputs(seed: int = 0, part: int = 0) -> dict:
    keys = jax.random.split(jax.random.key(seed), 4)
    part_splits = jax.random.split(jax.random.fold_in(keys[3], part), 4)
    return {
        "recorded": draw_recorded(jax.random.fold_in(jax.random.fold_in(keys[3], part), 71), part),
        "receiver_kernel": draw_receiver_kernel(jax.random.fold_in(jax.random.fold_in(keys[3], part), 71), part),
        "source_kernel": draw_source_kernel(jax.random.fold_in(jax.random.fold_in(keys[3], part), 71), part),
    }


def toeplitz(kernel, width):
    rows = jnp.arange(width, dtype=jnp.int32)[:, None]
    cols = jnp.arange(width, dtype=jnp.int32)[None, :]
    return kernel[:, cols - rows + width - 1]


def complex_dot(left, right):
    real_part = jnp.dot(left[0], right[0], preferred_element_type=jnp.float32) - jnp.dot(left[1], right[1], preferred_element_type=jnp.float32)
    imag_part = jnp.dot(left[0], right[1], preferred_element_type=jnp.float32) + jnp.dot(left[1], right[0], preferred_element_type=jnp.float32)
    return jnp.stack([real_part, imag_part])


def reference(recorded, receiver_kernel, source_kernel):
    prim_list = []
    mult_list = []
    for slot in range(FREQS):
        data = recorded[slot]
        data_b = data.astype(jnp.bfloat16)
        g_recv = toeplitz(receiver_kernel[slot], NR)
        g_src = toeplitz(source_kernel[slot], NS)
        focused = complex_dot(data_b, g_recv).astype(jnp.bfloat16)
        mult = complex_dot(g_src, focused).astype(jnp.bfloat16)
        mfl = mult.astype(jnp.float32)
        num_re = jnp.sum(mfl[0] * data[0] + mfl[1] * data[1])
        num_im = jnp.sum(mfl[0] * data[1] - mfl[1] * data[0])
        den = jnp.sum(mfl[0] * mfl[0] + mfl[1] * mfl[1]) + 1e-6
        fit_re = num_re / den
        fit_im = num_im / den
        prim_re = data[0] - (fit_re * mfl[0] - fit_im * mfl[1])
        prim_im = data[1] - (fit_re * mfl[1] + fit_im * mfl[0])
        prim_list.append(jnp.stack([prim_re, prim_im]))
        mult_list.append(mult)
    return jnp.stack(prim_list), jnp.stack(mult_list)
```

```python
import jax
import jax.numpy as jnp
from jax import lax
from jax.experimental import pallas as pl
from jax.experimental.pallas import tpu as pltpu
from jax.sharding import PartitionSpec as P

F32 = jnp.float32
BF16 = jnp.bfloat16
TILE = 256
VMEM_LIMIT = 56 * 1024 * 1024


def build_slab(kernel_ref, row_ref, slab_ref):
    taps = kernel_ref.shape[-1]
    length = taps + 1
    row_ref[:, :taps] = kernel_ref[0].astype(F32)
    for part in range(2):
        base = jnp.broadcast_to(row_ref[part : part + 1, :], (8, length))
        top = pltpu.roll(base, 1, 1, stride=1, stride_axis=0)
        for step in range(128 // 16):
            low = pltpu.roll(top, 16 * step, 1) if step else top
            high = pltpu.roll(top, 16 * step + 8, 1)
            slab_ref[part, 16 * step : 16 * step + 16, :] = jnp.concatenate([low, high], axis=0).astype(BF16)
        slab_ref[part, 128:256, 128:] = slab_ref[part, 0:128, : length - 128]


def focus_body(data_ref, kernel_ref, out_ref, row_ref, slab_ref, lhs_ref):
    rows, width = data_ref.shape[2], data_ref.shape[3]
    cols = out_ref.shape[2] // 2
    build_slab(kernel_ref, row_ref, slab_ref)
    lhs_ref[:rows] = data_ref[0, 0].astype(BF16)
    lhs_ref[rows:] = data_ref[0, 1].astype(BF16)
    lhs = lhs_ref[...]
    blocks = width // TILE
    for c in range(blocks):
        prods = []
        for part in range(2):
            rhs = jnp.concatenate(
                [slab_ref[part, :, width + TILE * (c - b) : width + TILE * (c - b) + TILE] for b in range(blocks)], axis=0
            )
            prods.append(jnp.dot(lhs, rhs, preferred_element_type=F32))
        re = (prods[0][:rows] - prods[1][rows:]).astype(BF16)
        im = (prods[1][:rows] + prods[0][rows:]).astype(BF16)
        for k in range(TILE // cols):
            dest = c * (TILE // cols) + k
            out_ref[dest, :, :cols] = re[:, k * cols : (k + 1) * cols]
            out_ref[dest, :, cols:] = im[:, k * cols : (k + 1) * cols]


def spread_body(kernel_ref, x_ref, out_ref, row_ref, slab_ref):
    sources, cols = x_ref.shape[0], x_ref.shape[1] // 2
    build_slab(kernel_ref, row_ref, slab_ref)
    for b in range(sources // TILE):
        first = sources - TILE * b
        pr = jnp.dot(slab_ref[0, :, first : first + sources], x_ref[...], preferred_element_type=F32)
        pi = jnp.dot(slab_ref[1, :, first : first + sources], x_ref[...], preferred_element_type=F32)
        out_ref[TILE * b : TILE * b + TILE, :cols] = (pr[:, :cols] - pi[:, cols:]).astype(BF16)
        out_ref[TILE * b : TILE * b + TILE, cols:] = (pr[:, cols:] + pi[:, :cols]).astype(BF16)


def fold(x):
    rows, width = x.shape
    x = x.reshape(rows // 8, 8, width).sum(axis=0)
    out = x[:, :128]
    for k in range(1, width // 128):
        out = out + x[:, 128 * k : 128 * k + 128]
    return out


def fit_body(data_ref, y_ref, mult_ref, sums_ref):
    panels, cols = y_ref.shape[0], y_ref.shape[2] // 2
    for q in range(panels):
        mult_ref[0, 0, :, q * cols : (q + 1) * cols] = y_ref[q, :, :cols]
        mult_ref[0, 1, :, q * cols : (q + 1) * cols] = y_ref[q, :, cols:]
    mr, mi = mult_ref[0, 0].astype(F32), mult_ref[0, 1].astype(F32)
    pr, pi = data_ref[0, 0], data_ref[0, 1]
    part = (fold(mr * pr + mi * pi), fold(mr * pi - mi * pr), fold(mr * mr + mi * mi))
    first = pl.program_id(0) == 0

    @pl.when(first)
    def _():
        for k in range(3):
            sums_ref[k] = part[k]

    @pl.when(jnp.logical_not(first))
    def _():
        for k in range(3):
            sums_ref[k] += part[k]


def subtract_body(data_ref, mult_ref, sums_ref, out_ref):
    num_re, num_im, energy = (jnp.sum(sums_ref[k], keepdims=True) for k in range(3))
    den = energy + 1e-6
    fit_re, fit_im = num_re / den, num_im / den
    mr, mi = mult_ref[0, 0].astype(F32), mult_ref[0, 1].astype(F32)
    out_ref[0, 0] = data_ref[0, 0] - (fit_re * mr - fit_im * mi)
    out_ref[0, 1] = data_ref[0, 1] - (fit_re * mi + fit_im * mr)


def params(**kw):
    return pltpu.CompilerParams(vmem_limit_bytes=VMEM_LIMIT, **kw)


def total(x, axis):
    n = lax.axis_size(axis)
    if n & (n - 1):
        return lax.psum(x, axis)
    step = n // 2
    while step:
        x = x + lax.ppermute(x, axis, [(k, k ^ step) for k in range(n)])
        step //= 2
    return x


def per_device(recorded, receiver_kernel, source_kernel):
    rows, width = recorded.shape[2], recorded.shape[3]
    panels = lax.axis_size("panel")
    sources = rows * panels
    cols = width // panels
    shape = jax.ShapeDtypeStruct

    focused = pl.pallas_call(
        focus_body,
        out_shape=shape((panels, rows, 2 * cols), BF16),
        scratch_shapes=[
            pltpu.VMEM((2, 2 * width), F32),
            pltpu.VMEM((2, TILE, 2 * width), BF16),
            pltpu.VMEM((2 * rows, width), BF16),
        ],
        compiler_params=params(),
        name="focus",
    )(recorded, receiver_kernel)
    columns = lax.all_to_all(focused, "panel", 0, 0, tiled=True).reshape(sources, 2 * cols)
    spread = pl.pallas_call(
        spread_body,
        out_shape=shape((sources, 2 * cols), BF16),
        scratch_shapes=[pltpu.VMEM((2, 2 * sources), F32), pltpu.VMEM((2, TILE, 2 * sources), BF16)],
        compiler_params=params(),
        name="spread",
    )(source_kernel, columns)
    back = lax.all_to_all(spread.reshape(panels, rows, 2 * cols), "panel", 0, 0, tiled=True)

    bm = 32
    data_spec = pl.BlockSpec((1, 2, bm, width), lambda i: (0, 0, i, 0))
    mult, sums = pl.pallas_call(
        fit_body,
        grid=(rows // bm,),
        in_specs=[data_spec, pl.BlockSpec((panels, bm, 2 * cols), lambda i: (0, i, 0))],
        out_specs=[data_spec, pl.BlockSpec((3, 8, 128), lambda i: (0, 0, 0))],
        out_shape=[shape((1, 2, rows, width), BF16), shape((3, 8, 128), F32)],
        compiler_params=params(),
        name="fit",
    )(recorded, back)
    sums = total(sums, "panel")
    prim = pl.pallas_call(
        subtract_body,
        grid=(rows // bm,),
        in_specs=[data_spec, data_spec, pl.BlockSpec((3, 8, 128), lambda i: (0, 0, 0))],
        out_specs=data_spec,
        out_shape=shape((1, 2, rows, width), F32),
        compiler_params=params(),
        name="subtract",
    )(recorded, mult, sums)
    return prim, mult


def solution(mesh):
    placed = (P("freq", None, "panel", None), P("freq", None, None), P("freq", None, None))
    return jax.shard_map(
        per_device,
        mesh=mesh,
        in_specs=placed,
        out_specs=(P("freq", None, "panel", None), P("freq", None, "panel", None)),
        check_vma=False,
    )
```

```python
import jax
import jax.numpy as jnp
from jax import lax
from jax.experimental import pallas as pl
from jax.experimental.pallas import tpu as pltpu
from jax.sharding import PartitionSpec as P

F32 = jnp.float32
BF16 = jnp.bfloat16
TILE = 256
VMEM_LIMIT = 56 * 1024 * 1024


def build_slab(kernel_ref, row_ref, slab_ref):
    taps = kernel_ref.shape[-1]
    length = taps + 1
    row_ref[:, :taps] = kernel_ref[0].astype(F32)
    for part in range(2):
        base = jnp.broadcast_to(row_ref[part : part + 1, :], (8, length))
        top = pltpu.roll(base, 1, 1, stride=1, stride_axis=0)
        for step in range(128 // 16):
            low = pltpu.roll(top, 16 * step, 1) if step else top
            high = pltpu.roll(top, 16 * step + 8, 1)
            slab_ref[part, 16 * step : 16 * step + 16, :] = jnp.concatenate([low, high], axis=0).astype(BF16)
        slab_ref[part, 128:256, 128:] = slab_ref[part, 0:128, : length - 128]


def focus_body(data_ref, kernel_ref, out_ref, row_ref, slab_ref, lhs_ref):
    rows, width = data_ref.shape[2], data_ref.shape[3]
    cols = out_ref.shape[2] // 2
    build_slab(kernel_ref, row_ref, slab_ref)
    lhs_ref[:rows] = data_ref[0, 0].astype(BF16)
    lhs_ref[rows:] = data_ref[0, 1].astype(BF16)
    lhs = lhs_ref[...]
    blocks = width // TILE
    for c in range(blocks):
        prods = []
        for part in range(2):
            rhs = jnp.concatenate(
                [slab_ref[part, :, width + TILE * (c - b) : width + TILE * (c - b) + TILE] for b in range(blocks)], axis=0
            )
            prods.append(jnp.dot(lhs, rhs, preferred_element_type=F32))
        re = (prods[0][:rows] - prods[1][rows:]).astype(BF16)
        im = (prods[1][:rows] + prods[0][rows:]).astype(BF16)
        for k in range(TILE // cols):
            dest = c * (TILE // cols) + k
            out_ref[dest, :, :cols] = re[:, k * cols : (k + 1) * cols]
            out_ref[dest, :, cols:] = im[:, k * cols : (k + 1) * cols]


def spread_body(kernel_ref, x_ref, out_ref, row_ref, slab_ref):
    sources, cols = x_ref.shape[0], x_ref.shape[1] // 2
    build_slab(kernel_ref, row_ref, slab_ref)
    for b in range(sources // TILE):
        first = sources - TILE * b
        pr = jnp.dot(slab_ref[0, :, first : first + sources], x_ref[...], preferred_element_type=F32)
        pi = jnp.dot(slab_ref[1, :, first : first + sources], x_ref[...], preferred_element_type=F32)
        out_ref[TILE * b : TILE * b + TILE, :cols] = (pr[:, :cols] - pi[:, cols:]).astype(BF16)
        out_ref[TILE * b : TILE * b + TILE, cols:] = (pr[:, cols:] + pi[:, :cols]).astype(BF16)


def fold(x):
    rows, width = x.shape
    x = x.reshape(rows // 8, 8, width).sum(axis=0)
    out = x[:, :128]
    for k in range(1, width // 128):
        out = out + x[:, 128 * k : 128 * k + 128]
    return out


def fit_body(data_ref, y_ref, sums_ref):
    panels, rows, cols = y_ref.shape[0], y_ref.shape[1], y_ref.shape[2] // 2
    strip = max(1, 128 // cols)
    acc = [jnp.zeros((8, 128), F32)] * 3
    for q in range(0, panels, strip):
        at = slice(q * cols, (q + strip) * cols)
        mr = jnp.concatenate([y_ref[q + k, :, :cols] for k in range(strip)], axis=1).astype(F32)
        mi = jnp.concatenate([y_ref[q + k, :, cols:] for k in range(strip)], axis=1).astype(F32)
        pr, pi = data_ref[0, 0, :, at], data_ref[0, 1, :, at]
        acc[0] += fold(mr * pr + mi * pi)
        acc[1] += fold(mr * pi - mi * pr)
        acc[2] += fold(mr * mr + mi * mi)
    for k in range(3):
        sums_ref[k] = acc[k]


def subtract_body(data_ref, y_ref, *refs):
    sums_refs, (out_ref, mult_ref) = refs[:-2], refs[-2:]
    panels, cols = y_ref.shape[0], y_ref.shape[2] // 2
    bm = out_ref.shape[2]
    sums = sums_refs[0][...]
    for ref in sums_refs[1:]:
        sums = sums + ref[...]
    num_re, num_im, energy = (jnp.sum(sums[k], keepdims=True) for k in range(3))
    den = energy + 1e-6
    fit_re, fit_im = num_re / den, num_im / den
    at = pl.ds(pl.multiple_of(pl.program_id(0) * bm, bm), bm)
    for q in range(panels):
        lanes = slice(q * cols, (q + 1) * cols)
        mult_ref[0, 0, :, lanes] = y_ref[q, at, :cols]
        mult_ref[0, 1, :, lanes] = y_ref[q, at, cols:]
    mr, mi = mult_ref[0, 0].astype(F32), mult_ref[0, 1].astype(F32)
    out_ref[0, 0] = data_ref[0, 0, at] - (fit_re * mr - fit_im * mi)
    out_ref[0, 1] = data_ref[0, 1, at] - (fit_re * mi + fit_im * mr)


def params(**kw):
    return pltpu.CompilerParams(vmem_limit_bytes=VMEM_LIMIT, **kw)


def small():
    return pltpu.CompilerParams(vmem_limit_bytes=16 * 1024 * 1024)


def partials(x, axis):
    n = lax.axis_size(axis)
    if n & (n - 1):
        return [lax.psum(x, axis)]
    terms, span = [x], n
    while span > 1:
        radix = min(4, span)
        span //= radix
        x = terms[0]
        for term in terms[1:]:
            x = x + term
        terms = [x] + [
            lax.ppermute(x, axis, [(k, k ^ (span * d)) for k in range(n)]) for d in range(1, radix)
        ]
    return terms


def per_device(recorded, receiver_kernel, source_kernel):
    rows, width = recorded.shape[2], recorded.shape[3]
    panels = lax.axis_size("panel")
    sources = rows * panels
    cols = width // panels
    shape = jax.ShapeDtypeStruct

    focused = pl.pallas_call(
        focus_body,
        out_shape=shape((panels, rows, 2 * cols), BF16),
        scratch_shapes=[
            pltpu.VMEM((2, 2 * width), F32),
            pltpu.VMEM((2, TILE, 2 * width), BF16),
            pltpu.VMEM((2 * rows, width), BF16),
        ],
        compiler_params=params(),
        name="focus",
    )(recorded, receiver_kernel)
    columns = lax.all_to_all(focused, "panel", 0, 0, tiled=True).reshape(sources, 2 * cols)
    spread = pl.pallas_call(
        spread_body,
        out_shape=shape((sources, 2 * cols), BF16),
        scratch_shapes=[pltpu.VMEM((2, 2 * sources), F32), pltpu.VMEM((2, TILE, 2 * sources), BF16)],
        compiler_params=params(),
        name="spread",
    )(source_kernel, columns)
    back = lax.all_to_all(spread.reshape(panels, rows, 2 * cols), "panel", 0, 0, tiled=True)

    resident = pl.BlockSpec(memory_space=pltpu.VMEM)
    sums = pl.pallas_call(
        fit_body,
        in_specs=[resident, resident],
        out_shape=shape((3, 8, 128), F32),
        compiler_params=small(),
        name="fit",
    )(recorded, back)
    terms = partials(sums, "panel")
    bm = 32
    block = pl.BlockSpec((1, 2, bm, width), lambda i: (0, 0, i, 0))
    return pl.pallas_call(
        subtract_body,
        grid=(rows // bm,),
        in_specs=[resident, resident] + [pl.BlockSpec((3, 8, 128), lambda i: (0, 0, 0))] * len(terms),
        out_specs=[block, block],
        out_shape=[shape((1, 2, rows, width), F32), shape((1, 2, rows, width), BF16)],
        compiler_params=small(),
        name="subtract",
    )(recorded, back, *terms)


def solution(mesh):
    placed = (P("freq", None, "panel", None), P("freq", None, None), P("freq", None, None))
    return jax.shard_map(
        per_device,
        mesh=mesh,
        in_specs=placed,
        out_specs=(P("freq", None, "panel", None), P("freq", None, "panel", None)),
        check_vma=False,
    )
```

```python
import functools

import jax
import jax.numpy as jnp
from jax import lax
from jax.experimental import pallas as pl
from jax.experimental.pallas import tpu as pltpu
from jax.sharding import PartitionSpec as P


F32 = jnp.float32
BF16 = jnp.bfloat16
TILE = 256
VMEM_LIMIT = 56 * 1024 * 1024


def build_slab(kernel_ref, row_ref, slab_ref):
    taps = kernel_ref.shape[-1]
    length = taps + 1
    row_ref[:, :taps] = kernel_ref[0].astype(F32)
    for part in range(2):
        base = jnp.broadcast_to(row_ref[part : part + 1, :], (8, length))
        top = pltpu.roll(base, 1, 1, stride=1, stride_axis=0)
        for step in range(128 // 16):
            low = pltpu.roll(top, 16 * step, 1) if step else top
            high = pltpu.roll(top, 16 * step + 8, 1)
            slab_ref[part, 16 * step : 16 * step + 16, :] = jnp.concatenate([low, high], axis=0).astype(BF16)
        slab_ref[part, 128:256, 128:] = slab_ref[part, 0:128, : length - 128]


def focus_body(data_ref, kernel_ref, out_ref, row_ref, slab_ref, lhs_ref):
    rows, width = data_ref.shape[2], data_ref.shape[3]
    cols = out_ref.shape[2] // 2
    build_slab(kernel_ref, row_ref, slab_ref)
    lhs_ref[:rows] = data_ref[0, 0].astype(BF16)
    lhs_ref[rows:] = data_ref[0, 1].astype(BF16)
    lhs = lhs_ref[...]
    blocks = width // TILE
    for c in range(blocks):
        prods = []
        for part in range(2):
            rhs = jnp.concatenate(
                [slab_ref[part, :, width + TILE * (c - b) : width + TILE * (c - b) + TILE] for b in range(blocks)], axis=0
            )
            prods.append(jnp.dot(lhs, rhs, preferred_element_type=F32))
        re = (prods[0][:rows] - prods[1][rows:]).astype(BF16)
        im = (prods[1][:rows] + prods[0][rows:]).astype(BF16)
        for k in range(TILE // cols):
            dest = c * (TILE // cols) + k
            out_ref[dest, :, :cols] = re[:, k * cols : (k + 1) * cols]
            out_ref[dest, :, cols:] = im[:, k * cols : (k + 1) * cols]


def spread_body(kernel_ref, x_ref, out_ref, row_ref, slab_ref):
    sources, cols = x_ref.shape[0], x_ref.shape[1] // 2
    build_slab(kernel_ref, row_ref, slab_ref)
    for b in range(sources // TILE):
        first = sources - TILE * b
        pr = jnp.dot(slab_ref[0, :, first : first + sources], x_ref[...], preferred_element_type=F32)
        pi = jnp.dot(slab_ref[1, :, first : first + sources], x_ref[...], preferred_element_type=F32)
        out_ref[TILE * b : TILE * b + TILE, :cols] = (pr[:, :cols] - pi[:, cols:]).astype(BF16)
        out_ref[TILE * b : TILE * b + TILE, cols:] = (pr[:, cols:] + pi[:, :cols]).astype(BF16)


def fold(x):
    rows, width = x.shape
    x = x.reshape(rows // 8, 8, width).sum(axis=0)
    out = x[:, :128]
    for k in range(1, width // 128):
        out = out + x[:, 128 * k : 128 * k + 128]
    return out


def fit_body(data_ref, y_ref, sums_ref):
    panels, cols = y_ref.shape[0], y_ref.shape[2] // 2
    strip = max(1, 128 // cols)
    acc = [jnp.zeros((8, 128), F32)] * 3
    for q in range(0, panels, strip):
        at = slice(q * cols, (q + strip) * cols)
        mr = jnp.concatenate([y_ref[q + k, :, :cols] for k in range(strip)], axis=1).astype(F32)
        mi = jnp.concatenate([y_ref[q + k, :, cols:] for k in range(strip)], axis=1).astype(F32)
        pr, pi = data_ref[0, 0, :, at], data_ref[0, 1, :, at]
        acc[0] += fold(mr * pr + mi * pi)
        acc[1] += fold(mr * pi - mi * pr)
        acc[2] += fold(mr * mr + mi * mi)
    for k in range(3):
        sums_ref[k] = acc[k]


def subtract_body(data_ref, y_ref, *refs):
    sums_refs, (out_ref, mult_ref) = refs[:-2], refs[-2:]
    panels, cols = y_ref.shape[0], y_ref.shape[2] // 2
    bm = out_ref.shape[2]
    sums = sums_refs[0][...]
    for ref in sums_refs[1:]:
        sums = sums + ref[...]
    num_re, num_im, energy = (jnp.sum(sums[k], keepdims=True) for k in range(3))
    den = energy + 1e-6
    fit_re, fit_im = num_re / den, num_im / den
    at = pl.ds(pl.multiple_of(pl.program_id(0) * bm, bm), bm)
    for q in range(panels):
        lanes = slice(q * cols, (q + 1) * cols)
        mult_ref[0, 0, :, lanes] = y_ref[q, at, :cols]
        mult_ref[0, 1, :, lanes] = y_ref[q, at, cols:]
    mr, mi = mult_ref[0, 0].astype(F32), mult_ref[0, 1].astype(F32)
    out_ref[0, 0] = data_ref[0, 0, at] - (fit_re * mr - fit_im * mi)
    out_ref[0, 1] = data_ref[0, 1, at] - (fit_re * mi + fit_im * mr)


def params(**kw):
    return pltpu.CompilerParams(vmem_limit_bytes=VMEM_LIMIT, **kw)


def medium():
    return pltpu.CompilerParams(vmem_limit_bytes=32 * 1024 * 1024)


def small():
    return pltpu.CompilerParams(vmem_limit_bytes=16 * 1024 * 1024)


def partials(x, axis):
    n = lax.axis_size(axis)
    if n & (n - 1):
        return [lax.psum(x, axis)]
    terms, span = [x], n
    while span > 1:
        radix = min(4, span)
        span //= radix
        x = terms[0]
        for term in terms[1:]:
            x = x + term
        terms = [x] + [
            lax.ppermute(x, axis, [(k, k ^ (span * d)) for k in range(n)]) for d in range(1, radix)
        ]
    return terms


def plain(recorded, receiver_kernel, source_kernel):
    rows, width = recorded.shape[2], recorded.shape[3]
    panels = lax.axis_size("panel")
    sources = rows * panels
    cols = width // panels
    shape = jax.ShapeDtypeStruct

    focused = pl.pallas_call(
        focus_body,
        out_shape=shape((panels, rows, 2 * cols), BF16),
        scratch_shapes=[
            pltpu.VMEM((2, 2 * width), F32),
            pltpu.VMEM((2, TILE, 2 * width), BF16),
            pltpu.VMEM((2 * rows, width), BF16),
        ],
        compiler_params=params(),
        name="focus",
    )(recorded, receiver_kernel)
    columns = lax.all_to_all(focused, "panel", 0, 0, tiled=True).reshape(sources, 2 * cols)
    spread = pl.pallas_call(
        spread_body,
        out_shape=shape((sources, 2 * cols), BF16),
        scratch_shapes=[pltpu.VMEM((2, 2 * sources), F32), pltpu.VMEM((2, TILE, 2 * sources), BF16)],
        compiler_params=params(),
        name="spread",
    )(source_kernel, columns)
    back = lax.all_to_all(spread.reshape(panels, rows, 2 * cols), "panel", 0, 0, tiled=True)

    resident = pl.BlockSpec(memory_space=pltpu.VMEM)
    sums = pl.pallas_call(
        fit_body,
        in_specs=[resident, resident],
        out_shape=shape((3, 8, 128), F32),
        compiler_params=small(),
        name="fit",
    )(recorded, back)
    terms = partials(sums, "panel")
    bm = 32
    block = pl.BlockSpec((1, 2, bm, width), lambda i: (0, 0, i, 0))
    return pl.pallas_call(
        subtract_body,
        grid=(rows // bm,),
        in_specs=[resident, resident] + [pl.BlockSpec((3, 8, 128), lambda i: (0, 0, 0))] * len(terms),
        out_specs=[block, block],
        out_shape=[shape((1, 2, rows, width), F32), shape((1, 2, rows, width), BF16)],
        compiler_params=small(),
        name="subtract",
    )(recorded, back, *terms)


def narrow_slab(kernel_ref, row_ref, slab_ref):
    taps = kernel_ref.shape[-1]
    row_ref[:, :taps] = kernel_ref[0].astype(F32)
    for part in range(2):
        base = jnp.broadcast_to(row_ref[part : part + 1, :], (8, taps + 1))
        top = pltpu.roll(base, 1, 1, stride=1, stride_axis=0)
        for step in range(8):
            low = pltpu.roll(top, 16 * step, 1) if step else top
            high = pltpu.roll(top, 16 * step + 8, 1)
            slab_ref[part, 16 * step : 16 * step + 16, :] = jnp.concatenate([low, high], axis=0).astype(BF16)


def lane_half(shape):
    return lax.broadcasted_iota(jnp.int32, shape, 1) < shape[1] // 2


def interleave(re, im):
    low = lane_half(re.shape)
    return jnp.where(low, re, pltpu.roll(im, 64, 1)), jnp.where(low, pltpu.roll(re, 64, 1), im)


def load_lhs(data_ref, lhs_ref):
    rows = data_ref.shape[2]
    lhs_ref[:rows] = data_ref[0, 0].astype(BF16)
    lhs_ref[rows:] = data_ref[0, 1].astype(BF16)
    return lhs_ref[...]


def chip_lane(offset):
    return 128 * ((lax.axis_index("panel") // 2) ^ offset)


def aligned(start, size):
    return pl.ds(pl.multiple_of(start, 128), size)


def focus_b_body(data_ref, kernel_ref, out_ref, row_ref, slab_ref, lhs_ref):
    rows, width = data_ref.shape[2], data_ref.shape[3]
    narrow_slab(kernel_ref, row_ref, slab_ref)
    lhs = load_lhs(data_ref, lhs_ref)
    for c in range(width // TILE // 2):
        first = width + width // 2 + TILE * c
        prods = []
        for part in range(2):
            rhs = [slab_ref[part, :, first - 128 * r : first - 128 * r + TILE] for r in range(width // 128)]
            prods.append(jnp.dot(lhs, jnp.concatenate(rhs, axis=0), preferred_element_type=F32))
        re, im = prods[0][:rows] - prods[1][rows:], prods[1][:rows] + prods[0][rows:]
        for k in range(2):
            pair = interleave(re[:, 128 * k : 128 * k + 128], im[:, 128 * k : 128 * k + 128])
            out_ref[4 * c + 2 * k] = pair[0].astype(BF16)
            out_ref[4 * c + 2 * k + 1] = pair[1].astype(BF16)


def focus_a_body(data_ref, kernel_ref, *refs):
    out_refs, (row_ref, slab_ref, lhs_ref) = refs[:-3], refs[-3:]
    rows, width = data_ref.shape[2], data_ref.shape[3]
    narrow_slab(kernel_ref, row_ref, slab_ref)
    lhs = load_lhs(data_ref, lhs_ref)
    for o in range(len(out_refs) - 2, -1, -2):
        prods = []
        for part in range(2):
            cols = []
            for k in range(2):
                first = width + chip_lane(o + k)
                cols.append(
                    jnp.concatenate(
                        [slab_ref[part, :, aligned(first - 128 * r, 128)] for r in range(width // 128)], axis=0
                    )
                )
            prods.append(jnp.dot(lhs, jnp.concatenate(cols, axis=1), preferred_element_type=F32))
        re = (prods[0][:rows] - prods[1][rows:]).astype(BF16)
        im = (prods[1][:rows] + prods[0][rows:]).astype(BF16)
        for k in range(2):
            out_refs[o + k][:, :128] = re[:, 128 * k : 128 * k + 128]
            out_refs[o + k][:, 128:] = im[:, 128 * k : 128 * k + 128]


def spread_b_body(kernel_ref, x_ref, out_ref, row_ref, slab_ref, cat_ref):
    sources = x_ref.shape[0]
    narrow_slab(kernel_ref, row_ref, slab_ref)
    zeros = jnp.zeros((128, 128), BF16)
    cat_ref[:128, :128] = zeros
    cat_ref[128:, :128] = x_ref[...]
    cat_ref[:sources, 128:] = x_ref[...]
    cat_ref[sources:, 128:] = zeros
    cat = cat_ref[...]
    for b in range(0, sources // 128, 4):
        prods = []
        for part in range(2):
            lhs = []
            for k in range(2):
                first = sources - 128 * (b + 2 * k) - 128
                lhs.append(slab_ref[part, :, first : first + sources + 128])
            prods.append(jnp.dot(jnp.concatenate(lhs, axis=0), cat, preferred_element_type=F32))
        for k in range(2):
            real, imag = prods[0][:, 128 * k : 128 * k + 128], prods[1][:, 128 * k : 128 * k + 128]
            turned = pltpu.roll(imag, 64, 1)
            both = (real + jnp.where(lane_half(turned.shape), -turned, turned)).astype(BF16)
            for h in range(2):
                row = 128 * (b + 2 * h + k)
                out_ref[row : row + 128] = both[128 * h : 128 * h + 128]


def spread_a_body(kernel_ref, peer_ref, *refs):
    chips = peer_ref.shape[0]
    own_refs, out_refs, (row_ref, slab_ref, x_ref) = refs[:chips], refs[chips : 2 * chips], refs[2 * chips :]
    sources = 2 * chips * 128
    narrow_slab(kernel_ref, row_ref, slab_ref)
    for o in range(chips):
        x_ref[128 * o : 128 * o + 128] = own_refs[o][...]
        x_ref[128 * (chips + o) : 128 * (chips + o) + 128] = peer_ref[o]
    x = x_ref[...]
    me = lax.axis_index("panel")
    chip, turn = me // 2, 128 - 256 * (me % 2)
    for out in range(chips - 2, -1, -2):
        prods = []
        for part in range(2):
            lhs = []
            for k in range(2):
                here = sources - 256 * (chip ^ (out + k))
                blocks = [
                    slab_ref[part, :, aligned(here + 256 * (chip ^ o) + shift, 128)]
                    for shift in (0, turn)
                    for o in range(chips)
                ]
                lhs.append(jnp.concatenate(blocks, axis=1))
            prods.append(jnp.dot(jnp.concatenate(lhs, axis=0), x, preferred_element_type=F32))
        re = (prods[0][:, :128] - prods[1][:, 128:]).astype(BF16)
        im = (prods[0][:, 128:] + prods[1][:, :128]).astype(BF16)
        for k in range(2):
            out_refs[out + k][:, :128] = re[128 * k : 128 * k + 128]
            out_refs[out + k][:, 128:] = im[128 * k : 128 * k + 128]


def stack_body(after_ref, *refs):
    for o, ref in enumerate(refs[:-1]):
        refs[-1][o] = ref[...]


def fit_two_body(data_ref, b_ref, *refs):
    a_refs, sums_ref = refs[:-1], refs[-1]
    panels, width = b_ref.shape[0], data_ref.shape[3]
    acc = [jnp.zeros((8, 128), F32)] * 3

    def add(mr, mi, at):
        pr, pi = data_ref[0, 0, :, at], data_ref[0, 1, :, at]
        acc[0] += fold(mr * pr + mi * pi)
        acc[1] += fold(mr * pi - mi * pr)
        acc[2] += fold(mr * mr + mi * mi)

    for q in range(0, panels, 2):
        mr, mi = interleave(b_ref[q].astype(F32), b_ref[q + 1].astype(F32))
        add(mr, mi, pl.ds(width // 2 + 64 * q, 128))
    for o, a_ref in enumerate(a_refs):
        add(a_ref[:, :128].astype(F32), a_ref[:, 128:].astype(F32), aligned(chip_lane(o), 128))
    for k in range(3):
        sums_ref[k] = acc[k]


def subtract_two_body(chips, data_ref, b_ref, *refs):
    a_refs, sums_refs, (out_ref, mult_ref) = refs[:chips], refs[chips:-2], refs[-2:]
    panels, width = b_ref.shape[0], data_ref.shape[3]
    bm = out_ref.shape[2]
    sums = sums_refs[0][...]
    for ref in sums_refs[1:]:
        sums = sums + ref[...]
    num_re, num_im, energy = (jnp.sum(sums[k], keepdims=True) for k in range(3))
    den = energy + 1e-6
    fit_re, fit_im = num_re / den, num_im / den
    rows = pl.ds(pl.multiple_of(pl.program_id(0) * bm, bm), bm)

    def finish(mr, mi, at):
        mult_ref[0, 0, :, at] = mr.astype(BF16)
        mult_ref[0, 1, :, at] = mi.astype(BF16)
        out_ref[0, 0, :, at] = data_ref[0, 0, rows, at] - (fit_re * mr - fit_im * mi)
        out_ref[0, 1, :, at] = data_ref[0, 1, rows, at] - (fit_re * mi + fit_im * mr)

    for q in range(0, panels, 2):
        mr, mi = interleave(b_ref[q, rows].astype(F32), b_ref[q + 1, rows].astype(F32))
        finish(mr, mi, pl.ds(width // 2 + 64 * q, 128))
    for o, a_ref in enumerate(a_refs):
        finish(a_ref[rows, :128].astype(F32), a_ref[rows, 128:].astype(F32), aligned(chip_lane(o), 128))


def piped(recorded, receiver_kernel, source_kernel):
    rows, width = recorded.shape[2], recorded.shape[3]
    panels = lax.axis_size("panel")
    chips = panels // 2
    sources = rows * panels
    shape = jax.ShapeDtypeStruct
    resident = pl.BlockSpec(memory_space=pltpu.VMEM)
    piece = shape((rows, 256), BF16)

    def slabs(length):
        return [pltpu.VMEM((2, 2 * length), F32), pltpu.VMEM((2, 128, 2 * length), BF16)]

    def exchange(pieces):
        return [pieces[0]] + [
            lax.ppermute(pieces[o], "panel", [(k, k ^ (2 * o)) for k in range(panels)]) for o in range(1, chips)
        ]

    focused_b = pl.pallas_call(
        focus_b_body,
        out_shape=shape((panels, rows, 128), BF16),
        scratch_shapes=slabs(width) + [pltpu.VMEM((2 * rows, width), BF16)],
        compiler_params=medium(),
        name="focus_b",
    )(recorded, receiver_kernel)
    columns_b = lax.all_to_all(focused_b, "panel", 0, 0, tiled=True).reshape(sources, 128)
    focused_a = pl.pallas_call(
        focus_a_body,
        out_shape=[piece] * chips,
        scratch_shapes=slabs(width) + [pltpu.VMEM((2 * rows, width), BF16)],
        compiler_params=medium(),
        name="focus_a",
    )(recorded, receiver_kernel)
    own = exchange(focused_a)
    spread_b = pl.pallas_call(
        spread_b_body,
        in_specs=[pl.BlockSpec(), resident],
        out_shape=shape((sources, 128), BF16),
        scratch_shapes=slabs(sources) + [pltpu.VMEM((sources + 128, 256), BF16)],
        compiler_params=medium(),
        name="spread_b",
    )(source_kernel, columns_b)
    back_b = lax.all_to_all(spread_b.reshape(panels, rows, 128), "panel", 0, 0, tiled=True)
    stacked = pl.pallas_call(
        stack_body,
        in_specs=[pl.BlockSpec(memory_space=pl.ANY)] + [resident] * chips,
        out_shape=shape((chips, rows, 256), BF16),
        compiler_params=small(),
        name="stack",
    )(spread_b, *own)
    peer = lax.ppermute(stacked, "panel", [(k, k ^ 1) for k in range(panels)])
    spread_a = pl.pallas_call(
        spread_a_body,
        in_specs=[pl.BlockSpec()] + [resident] * (1 + chips),
        out_shape=[piece] * chips,
        scratch_shapes=slabs(sources) + [pltpu.VMEM((sources, 256), BF16)],
        compiler_params=medium(),
        name="spread_a",
    )(source_kernel, peer, *own)
    back_a = exchange(spread_a)

    sums = pl.pallas_call(
        fit_two_body,
        in_specs=[resident] * (2 + chips),
        out_shape=shape((3, 8, 128), F32),
        compiler_params=small(),
        name="fit",
    )(recorded, back_b, *back_a)
    terms = partials(sums, "panel")
    bm = 32
    block = pl.BlockSpec((1, 2, bm, width), lambda i: (0, 0, i, 0))
    return pl.pallas_call(
        functools.partial(subtract_two_body, chips),
        grid=(rows // bm,),
        in_specs=[resident] * (2 + chips) + [pl.BlockSpec((3, 8, 128), lambda i: (0, 0, 0))] * len(terms),
        out_specs=[block, block],
        out_shape=[shape((1, 2, rows, width), F32), shape((1, 2, rows, width), BF16)],
        compiler_params=small(),
        name="subtract",
    )(recorded, back_b, *back_a, *terms)


def overlapping(panels):
    return panels >= 4 and panels & (panels - 1) == 0


def per_device(recorded, receiver_kernel, source_kernel):
    rows, width = recorded.shape[2], recorded.shape[3]
    panels = lax.axis_size("panel")
    if rows == 128 and width == 128 * panels and overlapping(panels):
        return piped(recorded, receiver_kernel, source_kernel)
    return plain(recorded, receiver_kernel, source_kernel)


def solution(mesh):
    placed = (P("freq", None, "panel", None), P("freq", None, None), P("freq", None, None))
    return jax.shard_map(
        per_device,
        mesh=mesh,
        in_specs=placed,
        out_specs=(P("freq", None, "panel", None), P("freq", None, "panel", None)),
        check_vma=False,
    )
```

```python
import functools

import jax
import jax.numpy as jnp
from jax import lax
from jax.experimental import pallas as pl
from jax.experimental.pallas import tpu as pltpu
from jax.sharding import PartitionSpec as P


F32 = jnp.float32
BF16 = jnp.bfloat16
TILE = 256
VMEM_LIMIT = 56 * 1024 * 1024


def build_slab(kernel_ref, row_ref, slab_ref):
    taps = kernel_ref.shape[-1]
    length = taps + 1
    row_ref[:, :taps] = kernel_ref[0].astype(F32)
    for part in range(2):
        base = jnp.broadcast_to(row_ref[part : part + 1, :], (8, length))
        top = pltpu.roll(base, 1, 1, stride=1, stride_axis=0)
        for step in range(128 // 16):
            low = pltpu.roll(top, 16 * step, 1) if step else top
            high = pltpu.roll(top, 16 * step + 8, 1)
            slab_ref[part, 16 * step : 16 * step + 16, :] = jnp.concatenate([low, high], axis=0).astype(BF16)
        slab_ref[part, 128:256, 128:] = slab_ref[part, 0:128, : length - 128]


def focus_all_body(data_ref, kernel_ref, out_ref, row_ref, slab_ref, lhs_ref):
    rows, width = data_ref.shape[2], data_ref.shape[3]
    cols = out_ref.shape[2] // 2
    build_slab(kernel_ref, row_ref, slab_ref)
    lhs_ref[:rows] = data_ref[0, 0].astype(BF16)
    lhs_ref[rows:] = data_ref[0, 1].astype(BF16)
    lhs = lhs_ref[...]
    blocks = width // TILE
    for c in range(blocks):
        prods = []
        for part in range(2):
            rhs = jnp.concatenate(
                [slab_ref[part, :, width + TILE * (c - b) : width + TILE * (c - b) + TILE] for b in range(blocks)], axis=0
            )
            prods.append(jnp.dot(lhs, rhs, preferred_element_type=F32))
        re = (prods[0][:rows] - prods[1][rows:]).astype(BF16)
        im = (prods[1][:rows] + prods[0][rows:]).astype(BF16)
        for k in range(TILE // cols):
            dest = c * (TILE // cols) + k
            out_ref[dest, :, :cols] = re[:, k * cols : (k + 1) * cols]
            out_ref[dest, :, cols:] = im[:, k * cols : (k + 1) * cols]


def spread_body(kernel_ref, x_ref, out_ref, row_ref, slab_ref):
    sources, cols = x_ref.shape[0], x_ref.shape[1] // 2
    build_slab(kernel_ref, row_ref, slab_ref)
    for b in range(sources // TILE):
        first = sources - TILE * b
        pr = jnp.dot(slab_ref[0, :, first : first + sources], x_ref[...], preferred_element_type=F32)
        pi = jnp.dot(slab_ref[1, :, first : first + sources], x_ref[...], preferred_element_type=F32)
        out_ref[TILE * b : TILE * b + TILE, :cols] = (pr[:, :cols] - pi[:, cols:]).astype(BF16)
        out_ref[TILE * b : TILE * b + TILE, cols:] = (pr[:, cols:] + pi[:, :cols]).astype(BF16)


def fold(x):
    rows, width = x.shape
    x = x.reshape(rows // 8, 8, width).sum(axis=0)
    out = x[:, :128]
    for k in range(1, width // 128):
        out = out + x[:, 128 * k : 128 * k + 128]
    return out


def fit_body(data_ref, y_ref, sums_ref):
    panels, cols = y_ref.shape[0], y_ref.shape[2] // 2
    strip = max(1, 128 // cols)
    acc = [jnp.zeros((8, 128), F32)] * 3
    for q in range(0, panels, strip):
        at = slice(q * cols, (q + strip) * cols)
        mr = jnp.concatenate([y_ref[q + k, :, :cols] for k in range(strip)], axis=1).astype(F32)
        mi = jnp.concatenate([y_ref[q + k, :, cols:] for k in range(strip)], axis=1).astype(F32)
        pr, pi = data_ref[0, 0, :, at], data_ref[0, 1, :, at]
        acc[0] += fold(mr * pr + mi * pi)
        acc[1] += fold(mr * pi - mi * pr)
        acc[2] += fold(mr * mr + mi * mi)
    for k in range(3):
        sums_ref[k] = acc[k]


def subtract_body(data_ref, y_ref, *refs):
    sums_refs, (out_ref, mult_ref) = refs[:-2], refs[-2:]
    panels, cols = y_ref.shape[0], y_ref.shape[2] // 2
    bm = out_ref.shape[2]
    sums = sums_refs[0][...]
    for ref in sums_refs[1:]:
        sums = sums + ref[...]
    num_re, num_im, energy = (jnp.sum(sums[k], keepdims=True) for k in range(3))
    den = energy + 1e-6
    fit_re, fit_im = num_re / den, num_im / den
    at = pl.ds(pl.multiple_of(pl.program_id(0) * bm, bm), bm)
    for q in range(panels):
        lanes = slice(q * cols, (q + 1) * cols)
        mult_ref[0, 0, :, lanes] = y_ref[q, at, :cols]
        mult_ref[0, 1, :, lanes] = y_ref[q, at, cols:]
    mr, mi = mult_ref[0, 0].astype(F32), mult_ref[0, 1].astype(F32)
    out_ref[0, 0] = data_ref[0, 0, at] - (fit_re * mr - fit_im * mi)
    out_ref[0, 1] = data_ref[0, 1, at] - (fit_re * mi + fit_im * mr)


def params(**kw):
    return pltpu.CompilerParams(vmem_limit_bytes=VMEM_LIMIT, **kw)


def medium():
    return pltpu.CompilerParams(vmem_limit_bytes=32 * 1024 * 1024)


def small():
    return pltpu.CompilerParams(vmem_limit_bytes=16 * 1024 * 1024)


def partials(x, axis):
    n = lax.axis_size(axis)
    if n & (n - 1):
        return [lax.psum(x, axis)]
    terms, span = [x], n
    while span > 1:
        radix = min(4, span)
        span //= radix
        x = terms[0]
        for term in terms[1:]:
            x = x + term
        terms = [x] + [
            lax.ppermute(x, axis, [(k, k ^ (span * d)) for k in range(n)]) for d in range(1, radix)
        ]
    return terms


def plain(recorded, receiver_kernel, source_kernel):
    rows, width = recorded.shape[2], recorded.shape[3]
    panels = lax.axis_size("panel")
    sources = rows * panels
    cols = width // panels
    shape = jax.ShapeDtypeStruct

    focused = pl.pallas_call(
        focus_all_body,
        out_shape=shape((panels, rows, 2 * cols), BF16),
        scratch_shapes=[
            pltpu.VMEM((2, 2 * width), F32),
            pltpu.VMEM((2, TILE, 2 * width), BF16),
            pltpu.VMEM((2 * rows, width), BF16),
        ],
        compiler_params=params(),
        name="focus",
    )(recorded, receiver_kernel)
    columns = lax.all_to_all(focused, "panel", 0, 0, tiled=True).reshape(sources, 2 * cols)
    spread = pl.pallas_call(
        spread_body,
        out_shape=shape((sources, 2 * cols), BF16),
        scratch_shapes=[pltpu.VMEM((2, 2 * sources), F32), pltpu.VMEM((2, TILE, 2 * sources), BF16)],
        compiler_params=params(),
        name="spread",
    )(source_kernel, columns)
    back = lax.all_to_all(spread.reshape(panels, rows, 2 * cols), "panel", 0, 0, tiled=True)

    resident = pl.BlockSpec(memory_space=pltpu.VMEM)
    sums = pl.pallas_call(
        fit_body,
        in_specs=[resident, resident],
        out_shape=shape((3, 8, 128), F32),
        compiler_params=small(),
        name="fit",
    )(recorded, back)
    terms = partials(sums, "panel")
    bm = 32
    block = pl.BlockSpec((1, 2, bm, width), lambda i: (0, 0, i, 0))
    return pl.pallas_call(
        subtract_body,
        grid=(rows // bm,),
        in_specs=[resident, resident] + [pl.BlockSpec((3, 8, 128), lambda i: (0, 0, 0))] * len(terms),
        out_specs=[block, block],
        out_shape=[shape((1, 2, rows, width), F32), shape((1, 2, rows, width), BF16)],
        compiler_params=small(),
        name="subtract",
    )(recorded, back, *terms)


def narrow_slab(kernel_ref, row_ref, slab_ref):
    taps = kernel_ref.shape[-1]
    row_ref[:, :taps] = kernel_ref[0].astype(F32)
    for part in range(2):
        base = jnp.broadcast_to(row_ref[part : part + 1, :], (8, taps + 1))
        top = pltpu.roll(base, 1, 1, stride=1, stride_axis=0)
        for step in range(8):
            low = pltpu.roll(top, 16 * step, 1) if step else top
            high = pltpu.roll(top, 16 * step + 8, 1)
            slab_ref[part, 16 * step : 16 * step + 16, :] = jnp.concatenate([low, high], axis=0).astype(BF16)


def aligned(start, size):
    return pl.ds(pl.multiple_of(start, 128), size)


def turns(chips, parity, home=False):
    half = chips // 2
    near, far = [*range(2, half), 1], [*range(half, chips)]
    return far + near if bool(parity) != home else near + far


def chip_at(chips, position, other=False, home=False):
    me = lax.axis_index("panel")
    if position == chips - 1:
        return me // 2
    even, odd = turns(chips, 0, home)[position], turns(chips, 1, home)[position]
    parity = 1 - me % 2 if other else me % 2
    return (me // 2) ^ (even + parity * (odd - even))


def focus_columns(chips, offsets, slab_ref, lhs_ref, out_refs):
    rows, width = lhs_ref.shape[0] // 2, lhs_ref.shape[1]
    lhs = lhs_ref[...]
    for offset, out_ref in zip(offsets, out_refs):
        first = width + 256 * chip_at(chips, offset)
        prods = []
        for part in range(2):
            rhs = [slab_ref[part, :, aligned(first - 128 * r, 256)] for r in range(width // 128)]
            prods.append(jnp.dot(lhs, jnp.concatenate(rhs, axis=0), preferred_element_type=F32))
        out_ref[:, :256] = (prods[0][:rows] - prods[1][rows:]).astype(BF16)
        out_ref[:, 256:] = (prods[1][:rows] + prods[0][rows:]).astype(BF16)


def focus_first_body(chips, offsets, data_hbm, kernel_hbm, *refs):
    out_refs, (slab_ref, lhs_ref, row_ref, data_ref, kernel_ref, sems) = refs[: len(offsets)], refs[len(offsets) :]
    rows = data_ref.shape[2]
    taps_in = pltpu.make_async_copy(kernel_hbm, kernel_ref, sems.at[0])
    data_in = pltpu.make_async_copy(data_hbm, data_ref, sems.at[1])
    taps_in.start()
    data_in.start()
    taps_in.wait()
    narrow_slab(kernel_ref, row_ref, slab_ref)
    data_in.wait()
    lhs_ref[:rows] = data_ref[0, 0].astype(BF16)
    lhs_ref[rows:] = data_ref[0, 1].astype(BF16)
    focus_columns(chips, offsets, slab_ref, lhs_ref, out_refs)


def focus_rest_body(chips, offsets, slab_ref, lhs_ref, *out_refs):
    focus_columns(chips, offsets, slab_ref, lhs_ref, out_refs)


def stack_body(*refs):
    for k, ref in enumerate(refs[:-1]):
        refs[-1][k] = ref[...]


def source_products(chips, slab_ref, stacks, outs):
    length = slab_ref.shape[2] // 2
    turn = 128 - 256 * (lax.axis_index("panel") % 2)
    sides = [(refs[other], other, ins) for *refs, ins in stacks for other in (False, True)]
    x = jnp.concatenate([ref[k] for ref, _, ins in sides for k in range(len(ins))], axis=0)
    prods = []
    for part in range(2):
        lhs = []
        for out in outs:
            here = length - 256 * chip_at(chips, out, home=True)
            blocks = [
                slab_ref[part, :, aligned(here + 256 * chip_at(chips, k, other) + turn * other, 128)]
                for _, other, ins in sides
                for k in ins
            ]
            lhs.append(jnp.concatenate(blocks, axis=1))
        prods.append(jnp.dot(jnp.concatenate(lhs, axis=0), x, preferred_element_type=F32))
    return prods[0][:, :256] - prods[1][:, 256:], prods[0][:, 256:] + prods[1][:, :256]


def slab_body(kernel_ref, slab_ref, row_ref):
    narrow_slab(kernel_ref, row_ref, slab_ref)


def begin_first_body(chips, outs, early, slab_ref, own_ref, peer_ref, acc_ref):
    re, im = source_products(chips, slab_ref, [(own_ref, peer_ref, early)], outs)
    for h in range(2):
        acc_ref[h, :, :256] = re[128 * h : 128 * h + 128]
        acc_ref[h, :, 256:] = im[128 * h : 128 * h + 128]


def finish_first_body(chips, outs, late, slab_ref, own_ref, peer_ref, acc_ref, *out_refs):
    re, im = source_products(chips, slab_ref, [(own_ref, peer_ref, late)], outs)
    for h in range(2):
        out_refs[h][:, :256] = (acc_ref[h, :, :256] + re[128 * h : 128 * h + 128]).astype(BF16)
        out_refs[h][:, 256:] = (acc_ref[h, :, 256:] + im[128 * h : 128 * h + 128]).astype(BF16)


def finish_rest_body(chips, outs, early, late, slab_ref, own_ref, peer_ref, late_own_ref, late_peer_ref, *out_refs):
    stacks = [(own_ref, peer_ref, early), (late_own_ref, late_peer_ref, late)]
    for k in range(0, len(outs), 2):
        re, im = source_products(chips, slab_ref, stacks, outs[k : k + 2])
        for h in range(2):
            out_refs[k + h][:, :256] = re[128 * h : 128 * h + 128].astype(BF16)
            out_refs[k + h][:, 256:] = im[128 * h : 128 * h + 128].astype(BF16)


def fit_pieces_body(data_ref, *refs):
    piece_refs, sums_ref = refs[:-1], refs[-1]
    acc = [jnp.zeros((8, 128), F32)] * 3
    for offset, ref in enumerate(piece_refs):
        mr, mi = ref[:, :256].astype(F32), ref[:, 256:].astype(F32)
        at = aligned(256 * chip_at(len(piece_refs), offset, home=True), 256)
        pr, pi = data_ref[0, 0, :, at], data_ref[0, 1, :, at]
        acc[0] += fold(mr * pr + mi * pi)
        acc[1] += fold(mr * pi - mi * pr)
        acc[2] += fold(mr * mr + mi * mi)
    for k in range(3):
        sums_ref[k] = acc[k]


def subtract_pieces_body(chips, data_ref, *refs):
    piece_refs, sums_refs, (out_ref, mult_ref) = refs[:chips], refs[chips:-2], refs[-2:]
    bm = out_ref.shape[2]
    sums = sums_refs[0][...]
    for ref in sums_refs[1:]:
        sums = sums + ref[...]
    num_re, num_im, energy = (jnp.sum(sums[k], keepdims=True) for k in range(3))
    den = energy + 1e-6
    fit_re, fit_im = num_re / den, num_im / den
    rows = pl.ds(pl.multiple_of(pl.program_id(0) * bm, bm), bm)
    for offset, ref in enumerate(piece_refs):
        at = aligned(256 * chip_at(len(piece_refs), offset, home=True), 256)
        mult_ref[0, 0, :, at] = ref[rows, :256]
        mult_ref[0, 1, :, at] = ref[rows, 256:]
        mr, mi = ref[rows, :256].astype(F32), ref[rows, 256:].astype(F32)
        out_ref[0, 0, :, at] = data_ref[0, 0, rows, at] - (fit_re * mr - fit_im * mi)
        out_ref[0, 1, :, at] = data_ref[0, 1, rows, at] - (fit_re * mi + fit_im * mr)


def piped(recorded, receiver_kernel, source_kernel):
    rows, width = recorded.shape[2], recorded.shape[3]
    panels = lax.axis_size("panel")
    chips = panels // 2
    own = chips - 1
    first, rest = (0, 1), (own, *range(2, own))
    early, late = (own, *range(chips // 2 - 1)), tuple(range(chips // 2 - 1, own))
    sources = rows * panels
    shape = jax.ShapeDtypeStruct
    resident = pl.BlockSpec(memory_space=pltpu.VMEM)
    in_hbm = pl.BlockSpec(memory_space=pltpu.HBM)
    piece = shape((rows, 512), BF16)

    def hbm(x):
        return pltpu.with_memory_space_constraint(x, pltpu.HBM)

    def exchange(pieces, positions, name):
        got = {}
        for x, p in zip(pieces, positions):
            if p != own:
                pairs = [(k, k ^ (2 * turns(chips, k % 2, name == "home")[p])) for k in range(panels)]
                x = lax.ppermute(x, "panel", pairs)
            got[p] = x
        return got

    def swap(pieces):
        mine = pl.pallas_call(
            stack_body,
            in_specs=[resident] * len(pieces),
            out_shape=pltpu.VMEM((len(pieces), rows, 512), BF16),
            compiler_params=small(),
        )(*pieces)
        return mine, lax.ppermute(mine, "panel", [(k, k ^ 1) for k in range(panels)])

    *pieces, slab_r, lhs = pl.pallas_call(
        functools.partial(focus_first_body, chips, first),
        in_specs=[in_hbm, in_hbm],
        out_shape=[piece] * len(first)
        + [pltpu.VMEM((2, 128, 2 * width), BF16), pltpu.VMEM((2 * rows, width), BF16)],
        scratch_shapes=[
            pltpu.VMEM((2, 2 * width), F32),
            pltpu.VMEM(recorded.shape, F32),
            pltpu.VMEM(receiver_kernel.shape, BF16),
            pltpu.SemaphoreType.DMA((2,)),
        ],
        compiler_params=medium(),
        name="focus_first",
    )(hbm(recorded), hbm(receiver_kernel))
    got = exchange(pieces, first, "away")
    pieces = pl.pallas_call(
        functools.partial(focus_rest_body, chips, rest),
        in_specs=[resident] * 2,
        out_shape=[piece] * len(rest),
        compiler_params=medium(),
        name="focus_rest",
    )(slab_r, lhs)
    got |= exchange(pieces, rest, "away")
    early_own, early_peer = swap([got[o] for o in early])
    slab_s = pl.pallas_call(
        slab_body,
        in_specs=[pl.BlockSpec()],
        out_shape=pltpu.VMEM((2, 128, 2 * sources), BF16),
        scratch_shapes=[pltpu.VMEM((2, 2 * sources), F32)],
        compiler_params=medium(),
        name="slab_source",
    )(source_kernel)

    acc_first = pl.pallas_call(
        functools.partial(begin_first_body, chips, first, early),
        in_specs=[resident] * 3,
        out_shape=pltpu.VMEM((len(first), rows, 512), F32),
        compiler_params=medium(),
        name="begin_first",
    )(slab_s, early_own, early_peer)
    late_own, late_peer = swap([got[o] for o in late])
    pieces = pl.pallas_call(
        functools.partial(finish_first_body, chips, first, late),
        in_specs=[resident] * 4,
        out_shape=[piece] * len(first),
        compiler_params=medium(),
        name="finish_first",
    )(slab_s, late_own, late_peer, acc_first)
    home = exchange(pieces, first, "home")
    pieces = pl.pallas_call(
        functools.partial(finish_rest_body, chips, rest, early, late),
        in_specs=[resident] * 5,
        out_shape=[piece] * len(rest),
        compiler_params=medium(),
        name="finish_rest",
    )(slab_s, early_own, early_peer, late_own, late_peer)
    home |= exchange(pieces, rest, "home")
    back = [home[o] for o in range(chips)]

    sums = pl.pallas_call(
        fit_pieces_body,
        in_specs=[resident] * (1 + chips),
        out_shape=shape((3, 8, 128), F32),
        compiler_params=small(),
        name="fit",
    )(recorded, *back)
    terms = partials(sums, "panel")
    bm = 32
    block = pl.BlockSpec((1, 2, bm, width), lambda i: (0, 0, i, 0))
    return pl.pallas_call(
        functools.partial(subtract_pieces_body, chips),
        grid=(rows // bm,),
        in_specs=[resident] * (1 + chips) + [pl.BlockSpec((3, 8, 128), lambda i: (0, 0, 0))] * len(terms),
        out_specs=[block, block],
        out_shape=[shape((1, 2, rows, width), F32), shape((1, 2, rows, width), BF16)],
        compiler_params=small(),
        name="subtract",
    )(recorded, *back, *terms)


def overlapping(panels):
    return panels >= 8 and panels & (panels - 1) == 0


def per_device(recorded, receiver_kernel, source_kernel):
    rows, width = recorded.shape[2], recorded.shape[3]
    panels = lax.axis_size("panel")
    if rows == 128 and width == 128 * panels and overlapping(panels):
        return piped(recorded, receiver_kernel, source_kernel)
    return plain(recorded, receiver_kernel, source_kernel)


def solution(mesh):
    placed = (P("freq", None, "panel", None), P("freq", None, None), P("freq", None, None))
    return jax.shard_map(
        per_device,
        mesh=mesh,
        in_specs=placed,
        out_specs=(P("freq", None, "panel", None), P("freq", None, "panel", None)),
        check_vma=False,
    )
```

```python
import functools

import jax
import jax.numpy as jnp
from jax import lax
from jax.experimental import pallas as pl
from jax.experimental.pallas import tpu as pltpu
from jax.sharding import PartitionSpec as P


F32 = jnp.float32
BF16 = jnp.bfloat16
TILE = 256
VMEM_LIMIT = 56 * 1024 * 1024


def build_slab(kernel_ref, row_ref, slab_ref):
    taps = kernel_ref.shape[-1]
    length = taps + 1
    row_ref[:, :taps] = kernel_ref[0].astype(F32)
    for part in range(2):
        base = jnp.broadcast_to(row_ref[part : part + 1, :], (8, length))
        top = pltpu.roll(base, 1, 1, stride=1, stride_axis=0)
        for step in range(128 // 16):
            low = pltpu.roll(top, 16 * step, 1) if step else top
            high = pltpu.roll(top, 16 * step + 8, 1)
            slab_ref[part, 16 * step : 16 * step + 16, :] = jnp.concatenate([low, high], axis=0).astype(BF16)
        slab_ref[part, 128:256, 128:] = slab_ref[part, 0:128, : length - 128]


def focus_all_body(data_ref, kernel_ref, out_ref, row_ref, slab_ref, lhs_ref):
    rows, width = data_ref.shape[2], data_ref.shape[3]
    cols = out_ref.shape[2] // 2
    build_slab(kernel_ref, row_ref, slab_ref)
    lhs_ref[:rows] = data_ref[0, 0].astype(BF16)
    lhs_ref[rows:] = data_ref[0, 1].astype(BF16)
    lhs = lhs_ref[...]
    blocks = width // TILE
    for c in range(blocks):
        prods = []
        for part in range(2):
            rhs = jnp.concatenate(
                [slab_ref[part, :, width + TILE * (c - b) : width + TILE * (c - b) + TILE] for b in range(blocks)], axis=0
            )
            prods.append(jnp.dot(lhs, rhs, preferred_element_type=F32))
        re = (prods[0][:rows] - prods[1][rows:]).astype(BF16)
        im = (prods[1][:rows] + prods[0][rows:]).astype(BF16)
        for k in range(TILE // cols):
            dest = c * (TILE // cols) + k
            out_ref[dest, :, :cols] = re[:, k * cols : (k + 1) * cols]
            out_ref[dest, :, cols:] = im[:, k * cols : (k + 1) * cols]


def spread_body(kernel_ref, x_ref, out_ref, row_ref, slab_ref):
    sources, cols = x_ref.shape[0], x_ref.shape[1] // 2
    build_slab(kernel_ref, row_ref, slab_ref)
    for b in range(sources // TILE):
        first = sources - TILE * b
        pr = jnp.dot(slab_ref[0, :, first : first + sources], x_ref[...], preferred_element_type=F32)
        pi = jnp.dot(slab_ref[1, :, first : first + sources], x_ref[...], preferred_element_type=F32)
        out_ref[TILE * b : TILE * b + TILE, :cols] = (pr[:, :cols] - pi[:, cols:]).astype(BF16)
        out_ref[TILE * b : TILE * b + TILE, cols:] = (pr[:, cols:] + pi[:, :cols]).astype(BF16)


def fold(x):
    rows, width = x.shape
    x = x.reshape(rows // 8, 8, width).sum(axis=0)
    out = x[:, :128]
    for k in range(1, width // 128):
        out = out + x[:, 128 * k : 128 * k + 128]
    return out


def fit_body(data_ref, y_ref, sums_ref):
    panels, cols = y_ref.shape[0], y_ref.shape[2] // 2
    strip = max(1, 128 // cols)
    acc = [jnp.zeros((8, 128), F32)] * 3
    for q in range(0, panels, strip):
        at = slice(q * cols, (q + strip) * cols)
        mr = jnp.concatenate([y_ref[q + k, :, :cols] for k in range(strip)], axis=1).astype(F32)
        mi = jnp.concatenate([y_ref[q + k, :, cols:] for k in range(strip)], axis=1).astype(F32)
        pr, pi = data_ref[0, 0, :, at], data_ref[0, 1, :, at]
        acc[0] += fold(mr * pr + mi * pi)
        acc[1] += fold(mr * pi - mi * pr)
        acc[2] += fold(mr * mr + mi * mi)
    for k in range(3):
        sums_ref[k] = acc[k]


def subtract_body(data_ref, y_ref, *refs):
    sums_refs, (out_ref, mult_ref) = refs[:-2], refs[-2:]
    panels, cols = y_ref.shape[0], y_ref.shape[2] // 2
    bm = out_ref.shape[2]
    sums = sums_refs[0][...]
    for ref in sums_refs[1:]:
        sums = sums + ref[...]
    num_re, num_im, energy = (jnp.sum(sums[k], keepdims=True) for k in range(3))
    den = energy + 1e-6
    fit_re, fit_im = num_re / den, num_im / den
    at = pl.ds(pl.multiple_of(pl.program_id(0) * bm, bm), bm)
    for q in range(panels):
        lanes = slice(q * cols, (q + 1) * cols)
        mult_ref[0, 0, :, lanes] = y_ref[q, at, :cols]
        mult_ref[0, 1, :, lanes] = y_ref[q, at, cols:]
    mr, mi = mult_ref[0, 0].astype(F32), mult_ref[0, 1].astype(F32)
    out_ref[0, 0] = data_ref[0, 0, at] - (fit_re * mr - fit_im * mi)
    out_ref[0, 1] = data_ref[0, 1, at] - (fit_re * mi + fit_im * mr)


def params(**kw):
    return pltpu.CompilerParams(vmem_limit_bytes=VMEM_LIMIT, **kw)


def medium():
    return pltpu.CompilerParams(vmem_limit_bytes=32 * 1024 * 1024)


def small():
    return pltpu.CompilerParams(vmem_limit_bytes=16 * 1024 * 1024)


def partials(x, axis):
    n = lax.axis_size(axis)
    if n & (n - 1):
        return [lax.psum(x, axis)]
    terms, span = [x], n
    while span > 1:
        radix = min(4, span)
        span //= radix
        x = terms[0]
        for term in terms[1:]:
            x = x + term
        terms = [x] + [
            lax.ppermute(x, axis, [(k, k ^ (span * d)) for k in range(n)]) for d in range(1, radix)
        ]
    return terms


def plain(recorded, receiver_kernel, source_kernel):
    rows, width = recorded.shape[2], recorded.shape[3]
    panels = lax.axis_size("panel")
    sources = rows * panels
    cols = width // panels
    shape = jax.ShapeDtypeStruct

    focused = pl.pallas_call(
        focus_all_body,
        out_shape=shape((panels, rows, 2 * cols), BF16),
        scratch_shapes=[
            pltpu.VMEM((2, 2 * width), F32),
            pltpu.VMEM((2, TILE, 2 * width), BF16),
            pltpu.VMEM((2 * rows, width), BF16),
        ],
        compiler_params=params(),
        name="focus",
    )(recorded, receiver_kernel)
    columns = lax.all_to_all(focused, "panel", 0, 0, tiled=True).reshape(sources, 2 * cols)
    spread = pl.pallas_call(
        spread_body,
        out_shape=shape((sources, 2 * cols), BF16),
        scratch_shapes=[pltpu.VMEM((2, 2 * sources), F32), pltpu.VMEM((2, TILE, 2 * sources), BF16)],
        compiler_params=params(),
        name="spread",
    )(source_kernel, columns)
    back = lax.all_to_all(spread.reshape(panels, rows, 2 * cols), "panel", 0, 0, tiled=True)

    resident = pl.BlockSpec(memory_space=pltpu.VMEM)
    sums = pl.pallas_call(
        fit_body,
        in_specs=[resident, resident],
        out_shape=shape((3, 8, 128), F32),
        compiler_params=small(),
        name="fit",
    )(recorded, back)
    terms = partials(sums, "panel")
    bm = 32
    block = pl.BlockSpec((1, 2, bm, width), lambda i: (0, 0, i, 0))
    return pl.pallas_call(
        subtract_body,
        grid=(rows // bm,),
        in_specs=[resident, resident] + [pl.BlockSpec((3, 8, 128), lambda i: (0, 0, 0))] * len(terms),
        out_specs=[block, block],
        out_shape=[shape((1, 2, rows, width), F32), shape((1, 2, rows, width), BF16)],
        compiler_params=small(),
        name="subtract",
    )(recorded, back, *terms)


def narrow_slab(kernel_ref, row_ref, slab_ref):
    taps = kernel_ref.shape[-1]
    row_ref[:, :taps] = kernel_ref[0].astype(F32)
    for part in range(2):
        base = jnp.broadcast_to(row_ref[part : part + 1, :], (8, taps + 1))
        top = pltpu.roll(base, 1, 1, stride=1, stride_axis=0)
        for step in range(8):
            low = pltpu.roll(top, 16 * step, 1) if step else top
            high = pltpu.roll(top, 16 * step + 8, 1)
            slab_ref[part, 16 * step : 16 * step + 16, :] = jnp.concatenate([low, high], axis=0).astype(BF16)


def aligned(start, size):
    return pl.ds(pl.multiple_of(start, 128), size)


def turns(chips, parity, home=False):
    half = chips // 2
    near, far = [*range(2, half), 1], [*range(half, chips)]
    return far + near if bool(parity) != home else near + far


def chip_at(chips, position, other=False, home=False):
    me = lax.axis_index("panel")
    if position == chips - 1:
        return me // 2
    even, odd = turns(chips, 0, home)[position], turns(chips, 1, home)[position]
    parity = 1 - me % 2 if other else me % 2
    return (me // 2) ^ (even + parity * (odd - even))


def focus_columns(chips, offsets, slab_ref, lhs_ref, out_refs):
    rows, width = lhs_ref.shape[0] // 2, lhs_ref.shape[1]
    lhs = lhs_ref[...]
    for offset, out_ref in zip(offsets, out_refs):
        first = width + 256 * chip_at(chips, offset)
        prods = []
        for part in range(2):
            rhs = [slab_ref[part, :, aligned(first - 128 * r, 256)] for r in range(width // 128)]
            prods.append(jnp.dot(lhs, jnp.concatenate(rhs, axis=0), preferred_element_type=F32))
        out_ref[:, :256] = (prods[0][:rows] - prods[1][rows:]).astype(BF16)
        out_ref[:, 256:] = (prods[1][:rows] + prods[0][rows:]).astype(BF16)


def focus_first_body(chips, offsets, data_hbm, kernel_hbm, *refs):
    out_refs, (slab_ref, lhs_ref, row_ref, data_ref, kernel_ref, sems) = refs[: len(offsets)], refs[len(offsets) :]
    rows = data_ref.shape[2]
    taps_in = pltpu.make_async_copy(kernel_hbm, kernel_ref, sems.at[0])
    data_in = pltpu.make_async_copy(data_hbm, data_ref, sems.at[1])
    taps_in.start()
    data_in.start()
    taps_in.wait()
    narrow_slab(kernel_ref, row_ref, slab_ref)
    data_in.wait()
    lhs_ref[:rows] = data_ref[0, 0].astype(BF16)
    lhs_ref[rows:] = data_ref[0, 1].astype(BF16)
    focus_columns(chips, offsets, slab_ref, lhs_ref, out_refs)


def focus_rest_body(chips, offsets, slab_ref, lhs_ref, *out_refs):
    focus_columns(chips, offsets, slab_ref, lhs_ref, out_refs)


def stack_body(*refs):
    pieces, out_ref = refs[-1 - refs[-1].shape[0] : -1], refs[-1]
    for k, ref in enumerate(pieces):
        out_ref[k] = ref[...]


def source_products(chips, slab_ref, stacks, outs):
    length = slab_ref.shape[2] // 2
    turn = 128 - 256 * (lax.axis_index("panel") % 2)
    sides = [(refs[other], other, ins) for *refs, ins in stacks for other in (False, True)]
    x = jnp.concatenate([ref[k] for ref, _, ins in sides for k in range(len(ins))], axis=0)
    prods = []
    for part in range(2):
        lhs = []
        for out in outs:
            here = length - 256 * chip_at(chips, out, home=True)
            blocks = [
                slab_ref[part, :, aligned(here + 256 * chip_at(chips, k, other) + turn * other, 128)]
                for _, other, ins in sides
                for k in ins
            ]
            lhs.append(jnp.concatenate(blocks, axis=1))
        prods.append(jnp.dot(jnp.concatenate(lhs, axis=0), x, preferred_element_type=F32))
    return prods[0][:, :256] - prods[1][:, 256:], prods[0][:, 256:] + prods[1][:, :256]


def slab_body(kernel_ref, slab_ref, row_ref):
    narrow_slab(kernel_ref, row_ref, slab_ref)


def begin_body(chips, outs, early, slab_ref, own_ref, peer_ref, acc_ref):
    for k in range(0, len(outs), 2):
        re, im = source_products(chips, slab_ref, [(own_ref, peer_ref, early)], outs[k : k + 2])
        for h in range(2):
            acc_ref[k + h, :, :256] = re[128 * h : 128 * h + 128]
            acc_ref[k + h, :, 256:] = im[128 * h : 128 * h + 128]


def finish_body(chips, outs, late, slab_ref, own_ref, peer_ref, acc_ref, *out_refs):
    for k in range(0, len(outs), 2):
        re, im = source_products(chips, slab_ref, [(own_ref, peer_ref, late)], outs[k : k + 2])
        for h in range(2):
            out_refs[k + h][:, :256] = (acc_ref[k + h, :, :256] + re[128 * h : 128 * h + 128]).astype(BF16)
            out_refs[k + h][:, 256:] = (acc_ref[k + h, :, 256:] + im[128 * h : 128 * h + 128]).astype(BF16)


def fit_pieces_body(data_ref, *refs):
    piece_refs, sums_ref = refs[:-1], refs[-1]
    acc = [jnp.zeros((8, 128), F32)] * 3
    for offset, ref in enumerate(piece_refs):
        mr, mi = ref[:, :256].astype(F32), ref[:, 256:].astype(F32)
        at = aligned(256 * chip_at(len(piece_refs), offset, home=True), 256)
        pr, pi = data_ref[0, 0, :, at], data_ref[0, 1, :, at]
        acc[0] += fold(mr * pr + mi * pi)
        acc[1] += fold(mr * pi - mi * pr)
        acc[2] += fold(mr * mr + mi * mi)
    for k in range(3):
        sums_ref[k] = acc[k]


def deliver_body(*refs):
    piece_refs, mult_ref = refs[:-1], refs[-1]
    bm = mult_ref.shape[2]
    rows = pl.ds(pl.multiple_of(pl.program_id(0) * bm, bm), bm)
    for offset, ref in enumerate(piece_refs):
        at = aligned(256 * chip_at(len(piece_refs), offset, home=True), 256)
        mult_ref[0, 0, :, at] = ref[rows, :256]
        mult_ref[0, 1, :, at] = ref[rows, 256:]


def subtract_pieces_body(chips, data_ref, *refs):
    piece_refs, sums_refs, out_ref = refs[:chips], refs[chips:-1], refs[-1]
    bm = out_ref.shape[2]
    sums = sums_refs[0][...]
    for ref in sums_refs[1:]:
        sums = sums + ref[...]
    num_re, num_im, energy = (jnp.sum(sums[k], keepdims=True) for k in range(3))
    den = energy + 1e-6
    fit_re, fit_im = num_re / den, num_im / den
    rows = pl.ds(pl.multiple_of(pl.program_id(0) * bm, bm), bm)
    for offset, ref in enumerate(piece_refs):
        at = aligned(256 * chip_at(len(piece_refs), offset, home=True), 256)
        mr, mi = ref[rows, :256].astype(F32), ref[rows, 256:].astype(F32)
        out_ref[0, 0, :, at] = data_ref[0, 0, rows, at] - (fit_re * mr - fit_im * mi)
        out_ref[0, 1, :, at] = data_ref[0, 1, rows, at] - (fit_re * mi + fit_im * mr)


def piped(recorded, receiver_kernel, source_kernel):
    rows, width = recorded.shape[2], recorded.shape[3]
    panels = lax.axis_size("panel")
    chips = panels // 2
    half, own = chips // 2, chips - 1
    first, rest = (0, 1), (own, *range(2, own))
    early, late = (own, *range(chips // 2 - 1)), tuple(range(chips // 2 - 1, own))
    sources = rows * panels
    shape = jax.ShapeDtypeStruct
    resident = pl.BlockSpec(memory_space=pltpu.VMEM)
    in_hbm = pl.BlockSpec(memory_space=pltpu.HBM)
    piece = shape((rows, 512), BF16)

    def hbm(x):
        return pltpu.with_memory_space_constraint(x, pltpu.HBM)

    def exchange(pieces, positions, name):
        got = {}
        for x, p in zip(pieces, positions):
            if p != own:
                pairs = [(k, k ^ (2 * turns(chips, k % 2, name == "home")[p])) for k in range(panels)]
                x = lax.ppermute(x, "panel", pairs)
            got[p] = x
        return got

    def swap(pieces):
        mine = pl.pallas_call(
            stack_body,
            in_specs=[resident] * len(pieces),
            out_shape=pltpu.VMEM((half, rows, 512), BF16),
            compiler_params=small(),
        )(*pieces)
        return mine, lax.ppermute(mine, "panel", [(k, k ^ 1) for k in range(panels)])

    *pieces, slab_r, lhs = pl.pallas_call(
        functools.partial(focus_first_body, chips, first),
        in_specs=[in_hbm, in_hbm],
        out_shape=[piece] * len(first)
        + [pltpu.VMEM((2, 128, 2 * width), BF16), pltpu.VMEM((2 * rows, width), BF16)],
        scratch_shapes=[
            pltpu.VMEM((2, 2 * width), F32),
            pltpu.VMEM(recorded.shape, F32),
            pltpu.VMEM(receiver_kernel.shape, BF16),
            pltpu.SemaphoreType.DMA((2,)),
        ],
        compiler_params=medium(),
        name="focus_first",
    )(hbm(recorded), hbm(receiver_kernel))
    got = exchange(pieces, first, "away")
    pieces = pl.pallas_call(
        functools.partial(focus_rest_body, chips, rest),
        in_specs=[resident] * 2,
        out_shape=[piece] * len(rest),
        compiler_params=medium(),
        name="focus_rest",
    )(slab_r, lhs)
    got |= exchange(pieces, rest, "away")
    early_own, early_peer = swap([got[o] for o in early])
    slab_s = pl.pallas_call(
        slab_body,
        in_specs=[pl.BlockSpec()],
        out_shape=pltpu.VMEM((2, 128, 2 * sources), BF16),
        scratch_shapes=[pltpu.VMEM((2, 2 * sources), F32)],
        compiler_params=medium(),
        name="slab_source",
    )(source_kernel)

    def begin(outs):
        return pl.pallas_call(
            functools.partial(begin_body, chips, outs, early),
            in_specs=[resident] * 3,
            out_shape=pltpu.VMEM((len(outs), rows, 512), F32),
            compiler_params=medium(),
        )(slab_s, early_own, early_peer)

    def finish(outs, acc):
        return pl.pallas_call(
            functools.partial(finish_body, chips, outs, late),
            in_specs=[resident] * 4,
            out_shape=[piece] * len(outs),
            compiler_params=medium(),
        )(slab_s, late_own, late_peer, acc)

    acc_first, acc_rest = begin(first), begin(rest)
    late_own, late_peer = swap([acc_rest] + [got[o] for o in late])
    home = exchange(finish(first, acc_first), first, "home")
    home |= exchange(finish(rest, acc_rest), rest, "home")
    back = [home[o] for o in range(chips)]

    sums = pl.pallas_call(
        fit_pieces_body,
        in_specs=[resident] * (1 + chips),
        out_shape=shape((3, 8, 128), F32),
        compiler_params=small(),
        name="fit",
    )(recorded, *back)
    terms = partials(sums, "panel")
    bm = 64
    block = pl.BlockSpec((1, 2, bm, width), lambda i: (0, 0, i, 0))
    mult = pl.pallas_call(
        deliver_body,
        grid=(rows // bm,),
        in_specs=[resident] * chips,
        out_specs=block,
        out_shape=shape((1, 2, rows, width), BF16),
        compiler_params=small(),
        name="deliver",
    )(*back)
    prim = pl.pallas_call(
        functools.partial(subtract_pieces_body, chips),
        grid=(rows // bm,),
        in_specs=[resident] * (1 + chips) + [pl.BlockSpec((3, 8, 128), lambda i: (0, 0, 0))] * len(terms),
        out_specs=block,
        out_shape=shape((1, 2, rows, width), F32),
        compiler_params=small(),
        name="subtract",
    )(recorded, *back, *terms)
    return prim, mult


def overlapping(panels):
    return panels >= 8 and panels & (panels - 1) == 0


def per_device(recorded, receiver_kernel, source_kernel):
    rows, width = recorded.shape[2], recorded.shape[3]
    panels = lax.axis_size("panel")
    if rows == 128 and width == 128 * panels and overlapping(panels):
        return piped(recorded, receiver_kernel, source_kernel)
    return plain(recorded, receiver_kernel, source_kernel)


def solution(mesh):
    placed = (P("freq", None, "panel", None), P("freq", None, None), P("freq", None, None))
    return jax.shard_map(
        per_device,
        mesh=mesh,
        in_specs=placed,
        out_specs=(P("freq", None, "panel", None), P("freq", None, "panel", None)),
        check_vma=False,
    )
```

```python
import functools

import jax
import jax.numpy as jnp
from jax import lax
from jax.experimental import pallas as pl
from jax.experimental.pallas import tpu as pltpu
from jax.sharding import PartitionSpec as P


F32 = jnp.float32
BF16 = jnp.bfloat16
TILE = 256
VMEM_LIMIT = 56 * 1024 * 1024


def build_slab(kernel_ref, row_ref, slab_ref):
    taps = kernel_ref.shape[-1]
    length = taps + 1
    row_ref[:, :taps] = kernel_ref[0].astype(F32)
    for part in range(2):
        base = jnp.broadcast_to(row_ref[part : part + 1, :], (8, length))
        top = pltpu.roll(base, 1, 1, stride=1, stride_axis=0)
        for step in range(128 // 16):
            low = pltpu.roll(top, 16 * step, 1) if step else top
            high = pltpu.roll(top, 16 * step + 8, 1)
            slab_ref[part, 16 * step : 16 * step + 16, :] = jnp.concatenate([low, high], axis=0).astype(BF16)
        slab_ref[part, 128:256, 128:] = slab_ref[part, 0:128, : length - 128]


def focus_all_body(data_ref, kernel_ref, out_ref, row_ref, slab_ref, lhs_ref):
    rows, width = data_ref.shape[2], data_ref.shape[3]
    cols = out_ref.shape[2] // 2
    build_slab(kernel_ref, row_ref, slab_ref)
    lhs_ref[:rows] = data_ref[0, 0].astype(BF16)
    lhs_ref[rows:] = data_ref[0, 1].astype(BF16)
    lhs = lhs_ref[...]
    blocks = width // TILE
    for c in range(blocks):
        prods = []
        for part in range(2):
            rhs = jnp.concatenate(
                [slab_ref[part, :, width + TILE * (c - b) : width + TILE * (c - b) + TILE] for b in range(blocks)], axis=0
            )
            prods.append(jnp.dot(lhs, rhs, preferred_element_type=F32))
        re = (prods[0][:rows] - prods[1][rows:]).astype(BF16)
        im = (prods[1][:rows] + prods[0][rows:]).astype(BF16)
        for k in range(TILE // cols):
            dest = c * (TILE // cols) + k
            out_ref[dest, :, :cols] = re[:, k * cols : (k + 1) * cols]
            out_ref[dest, :, cols:] = im[:, k * cols : (k + 1) * cols]


def spread_body(kernel_ref, x_ref, out_ref, row_ref, slab_ref):
    sources, cols = x_ref.shape[0], x_ref.shape[1] // 2
    build_slab(kernel_ref, row_ref, slab_ref)
    for b in range(sources // TILE):
        first = sources - TILE * b
        pr = jnp.dot(slab_ref[0, :, first : first + sources], x_ref[...], preferred_element_type=F32)
        pi = jnp.dot(slab_ref[1, :, first : first + sources], x_ref[...], preferred_element_type=F32)
        out_ref[TILE * b : TILE * b + TILE, :cols] = (pr[:, :cols] - pi[:, cols:]).astype(BF16)
        out_ref[TILE * b : TILE * b + TILE, cols:] = (pr[:, cols:] + pi[:, :cols]).astype(BF16)


def fold(x):
    rows, width = x.shape
    x = x.reshape(rows // 8, 8, width).sum(axis=0)
    out = x[:, :128]
    for k in range(1, width // 128):
        out = out + x[:, 128 * k : 128 * k + 128]
    return out


def fit_body(data_ref, y_ref, sums_ref):
    panels, cols = y_ref.shape[0], y_ref.shape[2] // 2
    strip = max(1, 128 // cols)
    acc = [jnp.zeros((8, 128), F32)] * 3
    for q in range(0, panels, strip):
        at = slice(q * cols, (q + strip) * cols)
        mr = jnp.concatenate([y_ref[q + k, :, :cols] for k in range(strip)], axis=1).astype(F32)
        mi = jnp.concatenate([y_ref[q + k, :, cols:] for k in range(strip)], axis=1).astype(F32)
        pr, pi = data_ref[0, 0, :, at], data_ref[0, 1, :, at]
        acc[0] += fold(mr * pr + mi * pi)
        acc[1] += fold(mr * pi - mi * pr)
        acc[2] += fold(mr * mr + mi * mi)
    for k in range(3):
        sums_ref[k] = acc[k]


def subtract_body(data_ref, y_ref, *refs):
    sums_refs, (out_ref, mult_ref) = refs[:-2], refs[-2:]
    panels, cols = y_ref.shape[0], y_ref.shape[2] // 2
    bm = out_ref.shape[2]
    sums = sums_refs[0][...]
    for ref in sums_refs[1:]:
        sums = sums + ref[...]
    num_re, num_im, energy = (jnp.sum(sums[k], keepdims=True) for k in range(3))
    den = energy + 1e-6
    fit_re, fit_im = num_re / den, num_im / den
    at = pl.ds(pl.multiple_of(pl.program_id(0) * bm, bm), bm)
    for q in range(panels):
        lanes = slice(q * cols, (q + 1) * cols)
        mult_ref[0, 0, :, lanes] = y_ref[q, at, :cols]
        mult_ref[0, 1, :, lanes] = y_ref[q, at, cols:]
    mr, mi = mult_ref[0, 0].astype(F32), mult_ref[0, 1].astype(F32)
    out_ref[0, 0] = data_ref[0, 0, at] - (fit_re * mr - fit_im * mi)
    out_ref[0, 1] = data_ref[0, 1, at] - (fit_re * mi + fit_im * mr)


def params(**kw):
    return pltpu.CompilerParams(vmem_limit_bytes=VMEM_LIMIT, **kw)


def medium():
    return pltpu.CompilerParams(vmem_limit_bytes=32 * 1024 * 1024)


def small():
    return pltpu.CompilerParams(vmem_limit_bytes=16 * 1024 * 1024)


def partials(x, axis):
    n = lax.axis_size(axis)
    if n & (n - 1):
        return [lax.psum(x, axis)]
    terms, span = [x], n
    while span > 1:
        radix = min(4, span)
        span //= radix
        x = terms[0]
        for term in terms[1:]:
            x = x + term
        terms = [x] + [
            lax.ppermute(x, axis, [(k, k ^ (span * d)) for k in range(n)]) for d in range(1, radix)
        ]
    return terms


def plain(recorded, receiver_kernel, source_kernel):
    rows, width = recorded.shape[2], recorded.shape[3]
    panels = lax.axis_size("panel")
    sources = rows * panels
    cols = width // panels
    shape = jax.ShapeDtypeStruct

    focused = pl.pallas_call(
        focus_all_body,
        out_shape=shape((panels, rows, 2 * cols), BF16),
        scratch_shapes=[
            pltpu.VMEM((2, 2 * width), F32),
            pltpu.VMEM((2, TILE, 2 * width), BF16),
            pltpu.VMEM((2 * rows, width), BF16),
        ],
        compiler_params=params(),
        name="focus",
    )(recorded, receiver_kernel)
    columns = lax.all_to_all(focused, "panel", 0, 0, tiled=True).reshape(sources, 2 * cols)
    spread = pl.pallas_call(
        spread_body,
        out_shape=shape((sources, 2 * cols), BF16),
        scratch_shapes=[pltpu.VMEM((2, 2 * sources), F32), pltpu.VMEM((2, TILE, 2 * sources), BF16)],
        compiler_params=params(),
        name="spread",
    )(source_kernel, columns)
    back = lax.all_to_all(spread.reshape(panels, rows, 2 * cols), "panel", 0, 0, tiled=True)

    resident = pl.BlockSpec(memory_space=pltpu.VMEM)
    sums = pl.pallas_call(
        fit_body,
        in_specs=[resident, resident],
        out_shape=shape((3, 8, 128), F32),
        compiler_params=small(),
        name="fit",
    )(recorded, back)
    terms = partials(sums, "panel")
    bm = 32
    block = pl.BlockSpec((1, 2, bm, width), lambda i: (0, 0, i, 0))
    return pl.pallas_call(
        subtract_body,
        grid=(rows // bm,),
        in_specs=[resident, resident] + [pl.BlockSpec((3, 8, 128), lambda i: (0, 0, 0))] * len(terms),
        out_specs=[block, block],
        out_shape=[shape((1, 2, rows, width), F32), shape((1, 2, rows, width), BF16)],
        compiler_params=small(),
        name="subtract",
    )(recorded, back, *terms)


def narrow_slab(kernel_ref, row_ref, slab_ref):
    taps = kernel_ref.shape[-1]
    row_ref[:, :taps] = kernel_ref[0].astype(F32)
    for part in range(2):
        base = jnp.broadcast_to(row_ref[part : part + 1, :], (8, taps + 1))
        top = pltpu.roll(base, 1, 1, stride=1, stride_axis=0)
        for step in range(8):
            low = pltpu.roll(top, 16 * step, 1) if step else top
            high = pltpu.roll(top, 16 * step + 8, 1)
            slab_ref[part, 16 * step : 16 * step + 16, :] = jnp.concatenate([low, high], axis=0).astype(BF16)


def aligned(start, size):
    return pl.ds(pl.multiple_of(start, 128), size)


def turns(chips, parity, home=False):
    half = chips // 2
    near, far = [*range(1, half)], [*range(half, chips, 2), *range(half + 1, chips, 2)]
    return far + near if bool(parity) != home else near + far


def chip_at(chips, position, other=False, home=False):
    me = lax.axis_index("panel")
    if position == chips - 1:
        return me // 2
    even, odd = turns(chips, 0, home)[position], turns(chips, 1, home)[position]
    parity = 1 - me % 2 if other else me % 2
    return (me // 2) ^ (even + parity * (odd - even))


def focus_columns(chips, offsets, slab_ref, lhs_ref, out_refs):
    rows, width = lhs_ref.shape[0] // 2, lhs_ref.shape[1]
    lhs = lhs_ref[...]
    for offset, out_ref in zip(offsets, out_refs):
        first = width + 256 * chip_at(chips, offset)
        prods = []
        for part in range(2):
            rhs = [slab_ref[part, :, aligned(first - 128 * r, 256)] for r in range(width // 128)]
            prods.append(jnp.dot(lhs, jnp.concatenate(rhs, axis=0), preferred_element_type=F32))
        out_ref[:, :256] = (prods[0][:rows] - prods[1][rows:]).astype(BF16)
        out_ref[:, 256:] = (prods[1][:rows] + prods[0][rows:]).astype(BF16)


def focus_first_body(chips, offsets, data_hbm, kernel_hbm, *refs):
    out_refs, (slab_ref, lhs_ref, row_ref, data_ref, kernel_ref, sems) = refs[: len(offsets)], refs[len(offsets) :]
    rows = data_ref.shape[2]
    taps_in = pltpu.make_async_copy(kernel_hbm, kernel_ref, sems.at[0])
    data_in = pltpu.make_async_copy(data_hbm, data_ref, sems.at[1])
    taps_in.start()
    data_in.start()
    taps_in.wait()
    narrow_slab(kernel_ref, row_ref, slab_ref)
    data_in.wait()
    lhs_ref[:rows] = data_ref[0, 0].astype(BF16)
    lhs_ref[rows:] = data_ref[0, 1].astype(BF16)
    focus_columns(chips, offsets, slab_ref, lhs_ref, out_refs)


def focus_rest_body(chips, offsets, slab_ref, lhs_ref, *out_refs):
    focus_columns(chips, offsets, slab_ref, lhs_ref, out_refs)


def stack_body(*refs):
    pieces, out_ref = refs[-1 - refs[-1].shape[0] : -1], refs[-1]
    for k, ref in enumerate(pieces):
        out_ref[k] = ref[...]


def source_products(chips, slab_ref, stacks, outs):
    length = slab_ref.shape[2] // 2
    turn = 128 - 256 * (lax.axis_index("panel") % 2)
    sides = [(refs[other], other, ins) for *refs, ins in stacks for other in (False, True)]
    x = jnp.concatenate([ref[k] for ref, _, ins in sides for k in range(len(ins))], axis=0)
    prods = []
    for part in range(2):
        lhs = []
        for out in outs:
            here = length - 256 * chip_at(chips, out, home=True)
            blocks = [
                slab_ref[part, :, aligned(here + 256 * chip_at(chips, k, other) + turn * other, 128)]
                for _, other, ins in sides
                for k in ins
            ]
            lhs.append(jnp.concatenate(blocks, axis=1))
        prods.append(jnp.dot(jnp.concatenate(lhs, axis=0), x, preferred_element_type=F32))
    return prods[0][:, :256] - prods[1][:, 256:], prods[0][:, 256:] + prods[1][:, :256]


def slab_body(kernel_ref, slab_ref, row_ref):
    narrow_slab(kernel_ref, row_ref, slab_ref)


def begin_body(chips, outs, early, slab_ref, own_ref, peer_ref, acc_ref):
    for k in range(0, len(outs), 2):
        re, im = source_products(chips, slab_ref, [(own_ref, peer_ref, early)], outs[k : k + 2])
        for h in range(2):
            acc_ref[k + h, :, :256] = re[128 * h : 128 * h + 128]
            acc_ref[k + h, :, 256:] = im[128 * h : 128 * h + 128]


def finish_body(chips, outs, late, slab_ref, own_ref, peer_ref, acc_ref, *out_refs):
    for k in range(0, len(outs), 2):
        re, im = source_products(chips, slab_ref, [(own_ref, peer_ref, late)], outs[k : k + 2])
        for h in range(2):
            out_refs[k + h][:, :256] = (acc_ref[k + h, :, :256] + re[128 * h : 128 * h + 128]).astype(BF16)
            out_refs[k + h][:, 256:] = (acc_ref[k + h, :, 256:] + im[128 * h : 128 * h + 128]).astype(BF16)


def fit_pieces_body(data_ref, *refs):
    piece_refs, sums_ref = refs[:-1], refs[-1]
    acc = [jnp.zeros((8, 128), F32)] * 3
    for offset, ref in enumerate(piece_refs):
        mr, mi = ref[:, :256].astype(F32), ref[:, 256:].astype(F32)
        at = aligned(256 * chip_at(len(piece_refs), offset, home=True), 256)
        pr, pi = data_ref[0, 0, :, at], data_ref[0, 1, :, at]
        acc[0] += fold(mr * pr + mi * pi)
        acc[1] += fold(mr * pi - mi * pr)
        acc[2] += fold(mr * mr + mi * mi)
    for k in range(3):
        sums_ref[k] = acc[k]


def deliver_body(*refs):
    piece_refs, mult_ref = refs[:-1], refs[-1]
    bm = mult_ref.shape[2]
    rows = pl.ds(pl.multiple_of(pl.program_id(0) * bm, bm), bm)
    for offset, ref in enumerate(piece_refs):
        at = aligned(256 * chip_at(len(piece_refs), offset, home=True), 256)
        mult_ref[0, 0, :, at] = ref[rows, :256]
        mult_ref[0, 1, :, at] = ref[rows, 256:]


def subtract_pieces_body(chips, data_ref, *refs):
    piece_refs, sums_refs, out_ref = refs[:chips], refs[chips:-1], refs[-1]
    bm = out_ref.shape[2]
    sums = sums_refs[0][...]
    for ref in sums_refs[1:]:
        sums = sums + ref[...]
    num_re, num_im, energy = (jnp.sum(sums[k], keepdims=True) for k in range(3))
    den = energy + 1e-6
    fit_re, fit_im = num_re / den, num_im / den
    rows = pl.ds(pl.multiple_of(pl.program_id(0) * bm, bm), bm)
    for offset, ref in enumerate(piece_refs):
        at = aligned(256 * chip_at(len(piece_refs), offset, home=True), 256)
        mr, mi = ref[rows, :256].astype(F32), ref[rows, 256:].astype(F32)
        out_ref[0, 0, :, at] = data_ref[0, 0, rows, at] - (fit_re * mr - fit_im * mi)
        out_ref[0, 1, :, at] = data_ref[0, 1, rows, at] - (fit_re * mi + fit_im * mr)


def piped(recorded, receiver_kernel, source_kernel):
    rows, width = recorded.shape[2], recorded.shape[3]
    panels = lax.axis_size("panel")
    chips = panels // 2
    half, own = chips // 2, chips - 1
    first, rest = (0, 1), (own, *range(2, own))
    early, late = (own, *range(chips // 2 - 1)), tuple(range(chips // 2 - 1, own))
    sources = rows * panels
    shape = jax.ShapeDtypeStruct
    resident = pl.BlockSpec(memory_space=pltpu.VMEM)
    in_hbm = pl.BlockSpec(memory_space=pltpu.HBM)
    piece = shape((rows, 512), BF16)

    def hbm(x):
        return pltpu.with_memory_space_constraint(x, pltpu.HBM)

    def exchange(pieces, positions, name):
        got = {}
        for x, p in zip(pieces, positions):
            if p != own:
                pairs = [(k, k ^ (2 * turns(chips, k % 2, name == "home")[p])) for k in range(panels)]
                x = lax.ppermute(x, "panel", pairs)
            got[p] = x
        return got

    def swap(pieces):
        mine = pl.pallas_call(
            stack_body,
            in_specs=[resident] * len(pieces),
            out_shape=pltpu.VMEM((half, rows, 512), BF16),
            compiler_params=small(),
        )(*pieces)
        return mine, lax.ppermute(mine, "panel", [(k, k ^ 1) for k in range(panels)])

    *pieces, slab_r, lhs = pl.pallas_call(
        functools.partial(focus_first_body, chips, first),
        in_specs=[in_hbm, in_hbm],
        out_shape=[piece] * len(first)
        + [pltpu.VMEM((2, 128, 2 * width), BF16), pltpu.VMEM((2 * rows, width), BF16)],
        scratch_shapes=[
            pltpu.VMEM((2, 2 * width), F32),
            pltpu.VMEM(recorded.shape, F32),
            pltpu.VMEM(receiver_kernel.shape, BF16),
            pltpu.SemaphoreType.DMA((2,)),
        ],
        compiler_params=medium(),
        name="focus_first",
    )(hbm(recorded), hbm(receiver_kernel))
    got = exchange(pieces, first, "away")
    for group in ((2, 3), (*range(4, own), own)):
        pieces = pl.pallas_call(
            functools.partial(focus_rest_body, chips, group),
            in_specs=[resident] * 2,
            out_shape=[piece] * len(group),
            compiler_params=medium(),
        )(slab_r, lhs)
        got |= exchange(pieces, group, "away")
    early_own, early_peer = swap([got[o] for o in early])
    slab_s = pl.pallas_call(
        slab_body,
        in_specs=[pl.BlockSpec()],
        out_shape=pltpu.VMEM((2, 128, 2 * sources), BF16),
        scratch_shapes=[pltpu.VMEM((2, 2 * sources), F32)],
        compiler_params=medium(),
        name="slab_source",
    )(source_kernel)

    def begin(outs):
        return pl.pallas_call(
            functools.partial(begin_body, chips, outs, early),
            in_specs=[resident] * 3,
            out_shape=pltpu.VMEM((len(outs), rows, 512), F32),
            compiler_params=medium(),
        )(slab_s, early_own, early_peer)

    def finish(outs, acc):
        return pl.pallas_call(
            functools.partial(finish_body, chips, outs, late),
            in_specs=[resident] * 4,
            out_shape=[piece] * len(outs),
            compiler_params=medium(),
        )(slab_s, late_own, late_peer, acc)

    acc_first, acc_rest = begin(first), begin(rest)
    late_own, late_peer = swap([acc_rest] + [got[o] for o in late])
    home = exchange(finish(first, acc_first), first, "home")
    home |= exchange(finish(rest, acc_rest), rest, "home")
    back = [home[o] for o in range(chips)]

    sums = pl.pallas_call(
        fit_pieces_body,
        in_specs=[resident] * (1 + chips),
        out_shape=shape((3, 8, 128), F32),
        compiler_params=small(),
        name="fit",
    )(recorded, *back)
    terms = partials(sums, "panel")
    bm = 64
    block = pl.BlockSpec((1, 2, bm, width), lambda i: (0, 0, i, 0))
    mult = pl.pallas_call(
        deliver_body,
        grid=(rows // bm,),
        in_specs=[resident] * chips,
        out_specs=block,
        out_shape=shape((1, 2, rows, width), BF16),
        compiler_params=small(),
        name="deliver",
    )(*back)
    prim = pl.pallas_call(
        functools.partial(subtract_pieces_body, chips),
        grid=(rows // bm,),
        in_specs=[resident] * (1 + chips) + [pl.BlockSpec((3, 8, 128), lambda i: (0, 0, 0))] * len(terms),
        out_specs=block,
        out_shape=shape((1, 2, rows, width), F32),
        compiler_params=small(),
        name="subtract",
    )(recorded, *back, *terms)
    return prim, mult


def overlapping(panels):
    return panels >= 16 and panels & (panels - 1) == 0


def per_device(recorded, receiver_kernel, source_kernel):
    rows, width = recorded.shape[2], recorded.shape[3]
    panels = lax.axis_size("panel")
    if rows == 128 and width == 128 * panels and overlapping(panels):
        return piped(recorded, receiver_kernel, source_kernel)
    return plain(recorded, receiver_kernel, source_kernel)


def solution(mesh):
    placed = (P("freq", None, "panel", None), P("freq", None, None), P("freq", None, None))
    return jax.shard_map(
        per_device,
        mesh=mesh,
        in_specs=placed,
        out_specs=(P("freq", None, "panel", None), P("freq", None, "panel", None)),
        check_vma=False,
    )
```
